256 devices in a mesh: bead: 16 (over x, z_hi), space: 16 (over z_lo, y, core).
Axes of the slice: x: 4, y: 4, z: 8 (z_hi: 4, z_lo: 2; z = z_hi * 2 + z_lo), core: 2. Of those that a mesh axis runs over, the one named last changes fastest.
Arguments:
- positions: float32 [64, 3, 4096], P('bead', None, 'space'), may hold values from -1 to 17
- species: int32 [4096], P('space'), may hold values from 0 to 1
- neighbors: int32 [32, 4096], P(None, 'space'), may hold values from 0 to 383, as said below
- counts: int32 [4096], P('space'), may hold values from 1 to 32, as said below
- send_rows: int32 [2048], P('space'), may hold values from 0 to 255, as said below
- embed: float32 [2, 128], replicated, may hold values from -6 to 6
- w_radial: float32 [2, 8, 128], replicated, may hold values from -2 to 2
- w_msg: float32 [2, 128, 128], replicated, may hold values from -0.5 to 0.5
- w_upd: float32 [2, 128, 128], replicated, may hold values from -0.5 to 0.5
- w_out: float32 [128], replicated, may hold values from -0.5 to 0.5
Outputs:
- forces: float32 [64, 3, 4096], P('bead', None, 'space')
The draws below stay inside these ranges and needn't reach their ends.
Inputs may be any that keep to these rules, and one draw needn't show every extreme that they name: `neighbors`: entry n < 256 is the domain's own row n; 256 + s is the s-th left ghost and 320 + s the s-th right ghost. `counts`: slots of an atom below its count are live, the others padding. `send_rows`: each domain's first 64 entries are a permutation of its rows 0 to 63, the next 64 a permutation of its rows 192 to 255.
All inputs are finite; a program needn't handle non-finite values.
Results may differ from the reference program's by a relative error of at most 0.0003.
Values sent between devices are 32-bit elements; how exact they have to be, the bound alone decides.
A program may use at most 64 MiB of HBM per device.

```python
import jax
import jax.numpy as jnp
from jax import lax

P_SIZE = 64
PC = 16
CH = 128
NB = 8
SPECIES = 2
K = 32
LAYERS = 2
A_DEV = 256
GH = 64
NATOMS = 4096
N_SPACE = 16


def draw_positions(key, part):
    first_key, second_key, third_key = jax.random.split(jax.random.fold_in(key, 11), 3)
    atom_index = jnp.arange(NATOMS, dtype=jnp.int32)
    domain = (atom_index // A_DEV).astype(jnp.float32)
    within = (atom_index % A_DEV).astype(jnp.float32)
    jitter = jax.random.uniform(first_key, (NATOMS,), jnp.float32)
    across = jax.random.uniform(second_key, (2, NATOMS), jnp.float32)
    centre = jnp.concatenate([(domain + (within + jitter) / A_DEV)[None], across], axis=0)
    spread = 0.05 * jnp.clip(jax.random.normal(third_key, (P_SIZE, 3, NATOMS), jnp.float32), -6.0, 6.0)
    return (centre[None] + spread).astype(jnp.float32)


def draw_neighbors(key, part):
    domains = NATOMS // A_DEV
    first_key, second_key, third_key, fourth_key = jax.random.split(jax.random.fold_in(key, 23), 4)
    shape_now = (K, domains, A_DEV)
    stride = jax.random.randint(first_key, shape_now, 1, GH + 1)
    direction = jax.random.randint(second_key, shape_now, 0, 2) * 2 - 1
    target = jnp.arange(A_DEV, dtype=jnp.int32)[None, None, :] + stride * direction
    left_slot = A_DEV + jax.random.randint(third_key, shape_now, 0, GH)
    right_slot = A_DEV + GH + jax.random.randint(fourth_key, shape_now, 0, GH)
    picked = jnp.where(target < 0, left_slot, jnp.where(target >= A_DEV, right_slot, target))
    return picked.reshape(K, NATOMS).astype(jnp.int32)


def draw_counts(key, part):
    domains = NATOMS // A_DEV
    first_key, second_key, third_key = jax.random.split(jax.random.fold_in(key, 37), 3)
    ceilings = jax.random.randint(first_key, (domains,), K // 4, K + 1)
    heaviest = jax.random.randint(second_key, (), 0, domains)
    ceilings = jnp.where(jnp.arange(domains, dtype=jnp.int32) == heaviest, K, ceilings)
    spread = jax.random.randint(third_key, (domains, A_DEV), 0, K)
    result = 1 + spread % ceilings[:, None]
    result = result.at[:, 0].set(ceilings)
    return result.reshape(NATOMS).astype(jnp.int32)


def draw_send_rows(key, part):
    domains = NATOMS // A_DEV
    first_key, second_key = jax.random.split(jax.random.fold_in(key, 53), 2)
    left_perm = jax.vmap(lambda sub_key: jax.random.permutation(sub_key, GH))(jax.random.split(first_key, domains))
    right_perm = jax.vmap(lambda sub_key: jax.random.permutation(sub_key, GH))(jax.random.split(second_key, domains))
    both_sides = jnp.concatenate([left_perm, A_DEV - GH + right_perm], axis=1)
    return both_sides.reshape(2 * GH * domains).astype(jnp.int32)


def place_ends(drawn, own_key, low, high):
    longest = drawn.shape.index(max(drawn.shape))
    spots = []
    for shift in (0, 1):
        where = [jax.random.randint(jax.random.fold_in(own_key, axis), (), 0, length) for axis, length in enumerate(drawn.shape)]
        where[longest] = (where[longest] + shift) % drawn.shape[longest]
        spots.append(tuple(where))
    return drawn.at[spots[0]].set(low).at[spots[1]].set(high)


def centred(own_key, dims, deviation, limit, held_as=jnp.bfloat16):
    return jnp.clip(deviation * jax.random.normal(own_key, dims, jnp.float32), -limit, limit).astype(held_as)


def setup_inputs(seed: int = 0) -> dict:
    key_of = jax.random.split(jax.random.key(seed), 11)
    return {
        "positions": draw_positions(jax.random.fold_in(key_of[10], 71), 0),
        "species": place_ends(jax.random.randint(key_of[1], (NATOMS,), 0, SPECIES), jax.random.fold_in(key_of[1], 1), 0, SPECIES - 1).astype(jnp.int32),
        "neighbors": draw_neighbors(jax.random.fold_in(key_of[10], 71), 0),
        "counts": draw_counts(jax.random.fold_in(key_of[10], 71), 0),
        "send_rows": draw_send_rows(jax.random.fold_in(key_of[10], 71), 0),
        "embed": centred(key_of[5], (SPECIES, CH), 1.0, 6.0, jnp.float32),
        "w_radial": centred(key_of[6], (LAYERS, NB, CH), NB ** -0.5, 2.0, jnp.float32),
        "w_msg": centred(key_of[7], (LAYERS, CH, CH), CH ** -0.5, 0.5, jnp.float32),
        "w_upd": centred(key_of[8], (LAYERS, CH, CH), CH ** -0.5, 0.5, jnp.float32),
        "w_out": centred(key_of[9], (CH,), CH ** -0.5, 0.5, jnp.float32),
    }


exact_mode = lax.Precision.HIGHEST
spacing_floor = 0.01
radial_width = 0.2
radial_reach = 1.5

def contraction(full_beads, reduced_beads):
    rowpos = jnp.arange(reduced_beads, dtype=jnp.float32)[:, None]
    colpos = jnp.arange(full_beads, dtype=jnp.float32)[None, :]
    phase_gap = rowpos / reduced_beads - colpos / full_beads
    running = jnp.ones_like(phase_gap)
    for harmonic in range(1, reduced_beads // 2):
        running = running + 2.0 * jnp.cos(2.0 * jnp.pi * harmonic * phase_gap)
    running = running + jnp.cos(jnp.pi * reduced_beads * phase_gap)
    return running / full_beads

def extend(stacked, sends):
    lent_pack = jax.vmap(lambda values, chosen: values[chosen])(stacked, sends)
    from_left = jnp.roll(lent_pack, 1, axis=0)[:, GH:]
    from_right = jnp.roll(lent_pack, -1, axis=0)[:, :GH]
    return jnp.concatenate([stacked, from_left, from_right], axis=1)

def bead_energy(points, onehot, neighbor_rows, live_slots, sends, embed, w_radial, w_msg, w_upd, w_out):
    extended = extend(points, sends)
    domain = jnp.arange(N_SPACE, dtype=jnp.int32)[:, None]
    rowidx = jnp.arange(A_DEV + 2 * GH, dtype=jnp.int32)[None, :]
    raised = ((domain == N_SPACE - 1) & (rowidx >= A_DEV + GH)).astype(jnp.float32)
    lowered = ((domain == 0) & (rowidx >= A_DEV) & (rowidx < A_DEV + GH)).astype(jnp.float32)
    extended = extended.at[:, :, 0].add(N_SPACE * (raised - lowered))
    near_points = jax.vmap(lambda values, chosen: values[chosen])(extended, neighbor_rows)
    displace = near_points - points[:, None]
    distance = jnp.sqrt(lax.optimization_barrier(jnp.sum(displace * displace, axis=-1)) + spacing_floor)
    centers = radial_reach * jnp.arange(NB, dtype=jnp.float32) / (NB - 1)
    offsets = (distance[..., None] - centers) / radial_width
    radial_basis = jnp.exp(-offsets * offsets)
    edge_scale = K ** (-0.5)
    hidden = jnp.einsum('sat,tc->sac', onehot, embed, precision=exact_mode)
    for layer_index in range(LAYERS):
        lent = jnp.einsum('sac,cd->sad', hidden, w_msg[layer_index], precision=exact_mode)
        lent_ext = extend(lent, sends)
        radial_w = jnp.einsum('skan,nc->skac', radial_basis, w_radial[layer_index], precision=exact_mode)
        near_rows = jax.vmap(lambda values, chosen: values[chosen])(lent_ext, neighbor_rows)
        message = edge_scale * lax.optimization_barrier(jnp.sum(live_slots[..., None] * radial_w * near_rows, axis=1))
        update = jnp.einsum('sac,cd->sad', message, w_upd[layer_index], precision=exact_mode)
        hidden = hidden + jax.nn.silu(update)
    return jnp.sum(hidden * w_out)

def reference(positions, species, neighbors, counts, send_rows, embed, w_radial, w_msg, w_upd, w_out):
    contract_table = contraction(P_SIZE, PC)
    reduced = jnp.einsum('kj,jcn->kcn', contract_table, positions, precision=exact_mode)
    points = reduced.reshape(PC, 3, N_SPACE, A_DEV).transpose(0, 2, 3, 1)
    onehot = (species.reshape(N_SPACE, A_DEV)[..., None] == jnp.arange(SPECIES, dtype=jnp.int32)).astype(jnp.float32)
    neighbor_rows = neighbors.reshape(K, N_SPACE, A_DEV).transpose(1, 0, 2)
    live_slots = (jnp.arange(K, dtype=jnp.int32)[None, :, None] < counts.reshape(N_SPACE, 1, A_DEV)).astype(jnp.float32)
    sends = send_rows.reshape(N_SPACE, 2 * GH)

    def one_bead(bead_points):
        slope = jax.grad(bead_energy)(bead_points, onehot, neighbor_rows, live_slots, sends, embed, w_radial, w_msg, w_upd, w_out)
        return -slope
    pulled = lax.map(one_bead, points)
    pulled = pulled.transpose(0, 3, 1, 2).reshape(PC, 3, NATOMS)
    return float(P_SIZE) / PC * jnp.einsum('kj,kcn->jcn', contract_table, pulled, precision=exact_mode)
```

```python
import functools
import math

import jax
import jax.numpy as jnp
from jax import lax
from jax.experimental import pallas as pl
from jax.experimental.pallas import tpu as pltpu
from jax.sharding import PartitionSpec as P

MESH = pl.DeviceIdType.MESH
HI = lax.Precision.HIGHEST
F32 = jnp.float32
BF16 = jnp.bfloat16

NB = 8
CH = 128
A = 256
G = 64
E = A + 2 * G
K = 32
H = 128
ROOT = math.sqrt(math.log2(math.e))
STEP = ROOT / 0.2
CENTERS = tuple(STEP * 1.5 * b / (NB - 1) for b in range(NB))
FLOOR = 0.01


def table_value(lag, beads, reduced):
    t = lag / beads
    total = 1.0 + math.cos(math.pi * reduced * t)
    for m in range(1, reduced // 2):
        total += 2.0 * math.cos(2.0 * math.pi * m * t)
    return total / beads


def split(v):
    hi = v.astype(BF16)
    lo = (v - hi.astype(F32)).astype(BF16)
    return hi, lo


def exact_dot(a, b):
    return jnp.dot(a, b, precision=HI, preferred_element_type=F32)


def exact_dot_nt(a, b):
    return lax.dot_general(
        a, b, (((1,), (1,)), ((), ())), precision=HI, preferred_element_type=F32
    )


def fast_dot(a, b):
    return jnp.dot(a, b, preferred_element_type=F32)


def kernel(
    nb, ns, own,
    pos_h, spc_h, nbr_h, cnt_h, snd_h, emb_h, wr_h, wm_h, wu_h, wo_h,
    out_ref,
    pos_v, spc_v, nbr_v, cnt_v, snd_v, emb_v, wr_v, wm_v, wu_v, wo_v,
    tx1, rx1, spc_l, spc_r, snd_l, snd_r, red_v, red_l, red_r,
    idx_v, cnt_mat, gcol, cen, w1bc, wu1t, wocol, p0, p0r, h0_v, slope0,
    ah_own, al_own, ah_gh, al_gh, z_v, rinv_v, l_v, x_v, xg_v, q_v, dl_own, dl_gh, r4_v,
    fold_v, tx5, r5_l, r5_r, tx6, rx6,
    load_sem, s1, r1, sa, ra, s2, r2, s3, r3, s4, r4, s5, r5, s6, r6,
):
    beads, reduced = nb * own, nb
    scale = K ** -0.5
    b = lax.axis_index("bead")
    d = lax.axis_index("space")
    left = lax.rem(d + (ns - 1), ns)
    right = lax.rem(d + 1, ns)
    peers = [lax.rem(b + lag, nb) for lag in range(nb)]

    def bead_copy(src, dst, ss, rs, lag):
        return pltpu.make_async_remote_copy(
            src_ref=src, dst_ref=dst, send_sem=ss, recv_sem=rs,
            device_id={"bead": peers[lag]}, device_id_type=MESH)

    def side_copy(src, dst, ss, rs, side):
        return pltpu.make_async_remote_copy(
            src_ref=src, dst_ref=dst, send_sem=ss, recv_sem=rs,
            device_id={"space": side}, device_id_type=MESH)

    barrier = pltpu.get_barrier_semaphore()
    for lag in range(1, nb):
        pl.semaphore_signal(barrier, inc=1, device_id={"bead": peers[lag]}, device_id_type=MESH)
    for side in (left, right):
        pl.semaphore_signal(barrier, inc=1, device_id={"space": side}, device_id_type=MESH)

    loads = []
    for i, (src, dst) in enumerate((
        (pos_h, pos_v), (spc_h, spc_v), (snd_h, snd_v), (nbr_h, nbr_v), (cnt_h, cnt_v),
        (emb_h, emb_v), (wr_h, wr_v), (wm_h, wm_v), (wu_h, wu_v), (wo_h, wo_v),
    )):
        copy = pltpu.make_async_copy(src, dst, load_sem.at[i])
        copy.start()
        loads.append(copy)

    loads[0].wait()
    packed = []
    for j in range(own):
        packed.append(jnp.concatenate(
            [pos_v[c, j : j + 1, half * H : half * H + H] for half in range(2) for c in range(3)], axis=0))
    for lag in range(nb):
        total = None
        for j in range(own):
            term = table_value(own * lag - j, beads, reduced) * packed[j]
            total = term if total is None else total + term
        tx1[lag] = total
    loads[1].wait()
    loads[2].wait()
    pl.semaphore_wait(barrier, nb + 1)

    first = [None] + [
        bead_copy(tx1.at[lag], rx1.at[lag], s1.at[lag], r1.at[lag], lag) for lag in range(1, nb)
    ]
    for lag in range(1, nb):
        first[lag].start()
    aux = [
        side_copy(spc_v, spc_r, sa.at[0], ra.at[0], left),
        side_copy(spc_v, spc_l, sa.at[1], ra.at[1], right),
        side_copy(snd_v, snd_r, sa.at[2], ra.at[2], left),
        side_copy(snd_v, snd_l, sa.at[3], ra.at[3], right),
    ]
    for copy in aux:
        copy.start()

    for copy in loads[3:]:
        copy.wait()
    n = nbr_v[...]
    n = jnp.where(n >= A + G, n - G, jnp.where(n >= A, n + G, n))
    slot = lax.broadcasted_iota(jnp.int32, (K, A), 0)
    idx_v[...] = jnp.where(slot < cnt_v[...], n, -1)

    def count_rows(i, carry):
        base = pl.multiple_of(i * 32, 32)
        row = lax.broadcasted_iota(jnp.int32, (32, A), 0) + base
        acc = jnp.zeros((32, A), F32)
        for k in range(K):
            acc = acc + jnp.where(idx_v[k : k + 1, :] == row, 1.0, 0.0)
        cnt_mat[pl.ds(base, 32), :] = acc
        return carry

    lax.fori_loop(0, E // 32, count_rows, 0)

    zeros6 = jnp.zeros((6, CH), F32)
    emb8 = jnp.concatenate([emb_v[...], zeros6], axis=0)
    table = exact_dot(emb8, wm_v[0])
    w0 = wr_v[0] * scale
    rows0 = jnp.concatenate([w0 * table[0:1], w0 * (table[1:2] - table[0:1])], axis=0)
    p0_now = exact_dot(rows0, wu_v[0])
    p0[...] = p0_now
    for j in range(2 * NB):
        p0r[pl.ds(8 * j, 8), :] = jnp.broadcast_to(p0_now[j : j + 1, :], (8, CH))
    w1 = wr_v[1] * scale
    w1t = jnp.transpose(jnp.concatenate([w1, jnp.zeros((CH - NB, CH), F32)], axis=0))
    for k in range(NB):
        w1bc[k] = jnp.broadcast_to(w1t[:, k : k + 1], (CH, H))
    wu1t[...] = jnp.transpose(wu_v[1])
    wot = jnp.transpose(jnp.broadcast_to(wo_v[...], (CH, CH)))
    wocol[...] = wot

    for copy in aux:
        copy.wait_recv()
    lane = lax.broadcasted_iota(jnp.int32, (1, H), 1)
    low = lane < G
    order = jnp.where(low, snd_r[...], snd_l[...] - (A - H))
    turn = jnp.where(
        lax.broadcasted_iota(jnp.int32, (H, H), 0) == order, 1.0, 0.0
    ).astype(BF16)
    cnt_mat[pl.ds(A, 2 * G), :] = fast_dot(turn, cnt_mat[pl.ds(A, 2 * G), :].astype(BF16))
    kind_own = spc_v[...].astype(F32)
    kind_gh = jnp.where(low, spc_r[0:1, :], spc_l[1:2, :]).astype(F32)
    zrest = jnp.zeros((CH - 4, H), F32)
    z3 = jnp.zeros((3, H), F32)
    for half in range(2):
        kcol = jnp.transpose(jnp.concatenate([z3, kind_own[half : half + 1], zrest], axis=0))
        h0_v[pl.ds(half * H, H), :] = jnp.where(
            kcol[:, 3:4] > 0.5, emb_v[1:2, :], emb_v[0:1, :])

    red = tx1[0]
    for lag in range(1, nb):
        first[lag].wait_recv()
        red = red + rx1[lag]
    red_v[...] = red
    second = [
        side_copy(red_v, red_r, s2.at[0], r2.at[0], left),
        side_copy(red_v, red_l, s2.at[1], r2.at[1], right),
    ]
    for copy in second:
        copy.start()
    cen[...] = jnp.concatenate(
        [jnp.concatenate([red[0:3], red[3:6]], axis=1), jnp.zeros((5, A), F32)], axis=0)
    for half in range(2):
        gcol[pl.ds(half * H, H), :] = jnp.transpose(jnp.concatenate(
            [red[3 * half : 3 * half + 3], kind_own[half : half + 1], zrest], axis=0))

    def pair_rows(start, ah, al, local):
        rows = 16

        def step(i, carry):
            base = pl.multiple_of(start + i * rows, rows)
            put = pl.multiple_of(i * rows, rows)
            col = gcol[pl.ds(base, rows), :]
            dx = col[:, 0:1] - cen[0:1, :]
            dy = col[:, 1:2] - cen[1:2, :]
            dz = col[:, 2:3] - cen[2:3, :]
            kind = jnp.broadcast_to(col[:, 3:4], (rows, A))
            square = dx * dx + dy * dy + dz * dz + FLOOR
            rinv = lax.rsqrt(square)
            x = square * rinv * STEP
            rinv_v[pl.ds(base, rows), :] = rinv
            c = cnt_mat[pl.ds(base, rows), :]
            sums = list(carry)
            for k in range(NB):
                off = x - CENTERS[k]
                a = c * jnp.exp2(-(off * off))
                hi, lo = split(a)
                ah[pl.ds(k * local + put, rows), :] = hi
                al[pl.ds(k * local + put, rows), :] = lo
                z_v[pl.ds(k * E + base, rows), :] = a * off
                s = a * kind
                sums[k] = sums[k] + (a[0:8] + a[8:16])
                sums[NB + k] = sums[NB + k] + (s[0:8] + s[8:16])
            return tuple(sums)

        return step

    sums = tuple(jnp.zeros((8, A), F32) for _ in range(2 * NB))
    sums = lax.fori_loop(0, A // 16, pair_rows(0, ah_own, al_own, A), sums)
    for copy in second:
        copy.wait_recv()
    ghost = jnp.where(low, red_r[0:3, :], red_l[3:6, :])
    shift_right = jnp.where(d == ns - 1, float(ns), 0.0)
    shift_left = jnp.where(d == 0, -float(ns), 0.0)
    shift = jnp.where(low, shift_right, shift_left)
    first_row = lax.broadcasted_iota(jnp.int32, (3, H), 0) == 0
    ghost = ghost + jnp.where(first_row, shift, 0.0)
    gcol[pl.ds(A, H), :] = jnp.transpose(jnp.concatenate([ghost, kind_gh, zrest], axis=0))
    sums = lax.fori_loop(0, 2 * G // 16, pair_rows(A, ah_gh, al_gh, 2 * G), sums)

    stacked = jnp.concatenate(sums, axis=0)
    u0 = exact_dot(jnp.transpose(stacked), p0r[...])
    sig0 = 1.0 / (1.0 + jnp.exp(-u0))
    slope0[...] = sig0 * (1.0 + u0 * (1.0 - sig0))
    h1 = h0_v[...] + u0 * sig0
    lent = exact_dot(h1, wm_v[1])
    l_v[pl.ds(0, A), :] = lent
    third = [
        side_copy(l_v.at[pl.ds(0, G)], l_v.at[pl.ds(A, G)], s3.at[0], r3.at[0], left),
        side_copy(l_v.at[pl.ds(A - G, G)], l_v.at[pl.ds(A + G, G)], s3.at[1], r3.at[1], right),
    ]
    for copy in third:
        copy.start()

    lt = jnp.transpose(lent)
    for k in range(NB):
        w = w1bc[k]
        hi, lo = split(lt * jnp.concatenate([w, w], axis=1))
        x_v[pl.ds(0, CH), pl.ds(k * A, A)] = hi
        x_v[pl.ds(CH, CH), pl.ds(k * A, A)] = lo
    both = fast_dot(x_v[...], ah_own[...])
    message = both[:CH] + both[CH:] + fast_dot(x_v[pl.ds(0, CH), :], al_own[...])
    for copy in third:
        copy.wait_recv()
    ltg = jnp.transpose(l_v[pl.ds(A, 2 * G), :])
    for k in range(NB):
        hi, lo = split(ltg * w1bc[k])
        xg_v[pl.ds(0, CH), pl.ds(k * 2 * G, 2 * G)] = hi
        xg_v[pl.ds(CH, CH), pl.ds(k * 2 * G, 2 * G)] = lo
    both = fast_dot(xg_v[...], ah_gh[...])
    message = message + (both[:CH] + both[CH:] + fast_dot(xg_v[pl.ds(0, CH), :], al_gh[...]))
    u1 = exact_dot(wu1t[...], message)
    sig1 = 1.0 / (1.0 + jnp.exp(-u1))
    wo2 = jnp.concatenate([wocol[...], wocol[...]], axis=1)
    gu1 = wo2 * (sig1 * (1.0 + u1 * (1.0 - sig1)))
    gm1t = exact_dot(wu_v[1], gu1)
    gm_hi, gm_lo = split(jnp.transpose(gm1t))
    gcat = jnp.concatenate([gm_hi, gm_lo], axis=1)

    def feature_grad(ah, al, local):
        total = None
        for k in range(NB):
            y = fast_dot(ah[pl.ds(k * local, local), :], gcat)
            y2 = fast_dot(al[pl.ds(k * local, local), :], gm_hi)
            term = (w1[k : k + 1, :]) * (y[:, :CH] + y[:, CH:] + y2)
            total = term if total is None else total + term
        return total

    dl_gh[...] = feature_grad(ah_gh, al_gh, 2 * G)
    fourth = [
        side_copy(dl_gh.at[pl.ds(0, G)], r4_v.at[pl.ds(0, G)], s4.at[0], r4.at[0], right),
        side_copy(dl_gh.at[pl.ds(G, G)], r4_v.at[pl.ds(G, G)], s4.at[1], r4.at[1], left),
    ]
    for copy in fourth:
        copy.start()
    dl_own[...] = feature_grad(ah_own, al_own, A)
    l_hi, l_lo = split(l_v[...])
    lcat = jnp.concatenate([l_hi, l_lo], axis=1)
    for k in range(NB):
        w = w1bc[k]
        hi, lo = split(gm1t * jnp.concatenate([w, w], axis=1))
        da = fast_dot(lcat, jnp.concatenate([hi, hi], axis=0)) + fast_dot(l_hi, lo)
        term = da * z_v[pl.ds(k * E, E), :]
        q_v[...] = term if k == 0 else q_v[...] + term
    for copy in fourth:
        copy.wait_recv()
    dl_own[pl.ds(0, G), :] = dl_own[pl.ds(0, G), :] + r4_v[pl.ds(0, G), :]
    dl_own[pl.ds(A - G, G), :] = dl_own[pl.ds(A - G, G), :] + r4_v[pl.ds(G, G), :]
    gh1 = wo_v[...] + exact_dot_nt(dl_own[...], wm_v[1])
    gu0 = gh1 * slope0[...]
    db = exact_dot_nt(p0[...], gu0)
    base_rows = db[0:NB]
    both_rows = db[0:NB] + db[NB : 2 * NB]

    factor = -2.0 / (0.2 * ROOT)

    def force_rows(start):
        rows = 16

        def step(i, carry):
            base = pl.multiple_of(start + i * rows, rows)
            col = gcol[pl.ds(base, rows), :]
            kind = jnp.broadcast_to(col[:, 3:4], (rows, A)) > 0.5
            q = q_v[pl.ds(base, rows), :]
            for k in range(NB):
                coef = jnp.where(kind, both_rows[k : k + 1, :], base_rows[k : k + 1, :])
                q = q + coef * z_v[pl.ds(k * E + base, rows), :]
            g = q * rinv_v[pl.ds(base, rows), :] * factor
            new = []
            for c in range(3):
                f = g * (col[:, c : c + 1] - cen[c : c + 1, :])
                fold_v[c, pl.ds(base, rows), :] = f[:, :H] + f[:, H:]
                new.append(carry[c] + (f[0:8] + f[8:16]))
            return tuple(new)

        return step

    def row_sums(start):
        return jnp.concatenate(
            [jnp.sum(jnp.transpose(fold_v[c, pl.ds(start, H), :]), axis=0, keepdims=True)
             for c in range(3)], axis=0)

    pulls = tuple(jnp.zeros((8, A), F32) for _ in range(3))
    pulls = lax.fori_loop(0, 2 * G // 16, force_rows(A), pulls)
    tx5[...] = row_sums(A)
    fifth = [
        side_copy(tx5, r5_l, s5.at[0], r5.at[0], right),
        side_copy(tx5, r5_r, s5.at[1], r5.at[1], left),
    ]
    for copy in fifth:
        copy.start()
    pulls = lax.fori_loop(0, A // 16, force_rows(0), pulls)
    centre = jnp.concatenate([jnp.sum(v, axis=0, keepdims=True) for v in pulls], axis=0)
    lower = centre[:, :H] - row_sums(0)
    upper = centre[:, H:] - row_sums(H)
    for copy in fifth:
        copy.wait_recv()
    lower = lower - jnp.where(low, r5_l[...], 0.0)
    upper = upper - jnp.where(low, 0.0, r5_r[...])
    pull = jnp.concatenate([lower, upper], axis=0)
    tx6[...] = pull
    last = [None] + [
        bead_copy(tx6, rx6.at[lag], s6.at[lag], r6.at[lag], lag) for lag in range(1, nb)
    ]
    for lag in range(1, nb):
        last[lag].start()
    ratio = beads / reduced
    totals = [ratio * table_value(-j, beads, reduced) * pull for j in range(own)]
    for lag in range(1, nb):
        last[lag].wait_recv()
        arrived = rx6[lag]
        for j in range(own):
            totals[j] = totals[j] + ratio * table_value(-own * lag - j, beads, reduced) * arrived
    for c in range(3):
        for half in range(2):
            row = 3 * half + c
            out_ref[c, :, half * H : half * H + H] = jnp.concatenate(
                [totals[j][row : row + 1] for j in range(own)], axis=0)
    for copy in first[1:] + aux + second + third + fourth + fifth + last[1:]:
        copy.wait_send()


def solution(mesh):
    nb, ns = mesh.shape["bead"], mesh.shape["space"]

    def on_device(positions, species, neighbors, counts, send_rows, embed, w_radial, w_msg, w_upd, w_out):
        own = positions.shape[0]
        vm = pltpu.VMEM
        dma = pltpu.SemaphoreType.DMA
        scratch = [
            vm((3, own, A), F32), vm((2, H), jnp.int32), vm((K, A), jnp.int32), vm((1, A), jnp.int32),
            vm((1, H), jnp.int32), vm((2, CH), F32), vm((2, NB, CH), F32), vm((2, CH, CH), F32),
            vm((2, CH, CH), F32), vm((1, CH), F32),
            vm((nb, 6, H), F32), vm((nb, 6, H), F32), vm((2, H), jnp.int32), vm((2, H), jnp.int32),
            vm((1, H), jnp.int32), vm((1, H), jnp.int32), vm((6, H), F32), vm((6, H), F32), vm((6, H), F32),
            vm((K, A), jnp.int32), vm((E, A), F32), vm((E, H), F32), vm((8, A), F32), vm((NB, CH, H), F32),
            vm((CH, CH), F32), vm((CH, CH), F32), vm((2 * NB, CH), F32), vm((16 * NB, CH), F32),
            vm((A, CH), F32), vm((A, CH), F32),
            vm((NB * A, A), BF16), vm((NB * A, A), BF16), vm((NB * 2 * G, A), BF16), vm((NB * 2 * G, A), BF16),
            vm((NB * E, A), F32), vm((E, A), F32), vm((E, CH), F32), vm((2 * CH, NB * A), BF16),
            vm((2 * CH, NB * 2 * G), BF16), vm((E, A), F32), vm((A, CH), F32), vm((2 * G, CH), F32),
            vm((2 * G, CH), F32),
            vm((3, E, H), F32), vm((3, H), F32), vm((3, H), F32), vm((3, H), F32), vm((6, H), F32),
            vm((nb, 6, H), F32),
            dma((10,)), dma((nb,)), dma((nb,)), dma((4,)), dma((4,)), dma((2,)), dma((2,)), dma((2,)), dma((2,)),
            dma((2,)), dma((2,)), dma((2,)), dma((2,)), dma((nb,)), dma((nb,)),
        ]
        forces = pl.pallas_call(
            functools.partial(kernel, nb, ns, own),
            out_shape=jax.ShapeDtypeStruct((3, own, A), F32),
            in_specs=[pl.BlockSpec(memory_space=pl.ANY)] * 10,
            out_specs=pl.BlockSpec(memory_space=pltpu.VMEM),
            scratch_shapes=scratch,
            compiler_params=pltpu.CompilerParams(collective_id=0, has_side_effects=True),
        )(
            positions.transpose(1, 0, 2), species.reshape(2, H), neighbors, counts.reshape(1, A), send_rows.reshape(1, H),
            embed, w_radial, w_msg, w_upd, w_out.reshape(1, CH),
        )
        return forces.transpose(1, 0, 2)

    return jax.shard_map(
        on_device,
        mesh=mesh,
        in_specs=(
            P("bead", None, "space"), P("space"), P(None, "space"), P("space"), P("space"),
            P(), P(), P(), P(), P(),
        ),
        out_specs=P("bead", None, "space"),
        check_vma=False,
    )
```

```python
import functools
import math

import jax
import jax.numpy as jnp
from jax import lax
from jax.experimental import pallas as pl
from jax.experimental.pallas import tpu as pltpu
from jax.sharding import PartitionSpec as P

MESH = pl.DeviceIdType.MESH
HI = lax.Precision.HIGHEST
F32 = jnp.float32
BF16 = jnp.bfloat16

NB = 8
CH = 128
A = 256
G = 64
E = A + 2 * G
K = 32
H = 128
ROOT = math.sqrt(math.log2(math.e))
STEP = ROOT / 0.2
CENTERS = tuple(STEP * 1.5 * b / (NB - 1) for b in range(NB))
FLOOR = 0.01
UNROLL = 2


def by_distance(nb):
    def far(lag):
        dz, dx = lag % 4, lag // 4
        return -(2 * min(dz, 4 - dz) + min(dx, 4 - dx))

    return sorted(range(1, nb), key=far)


def table_value(lag, beads, reduced):
    t = lag / beads
    total = 1.0 + math.cos(math.pi * reduced * t)
    for m in range(1, reduced // 2):
        total += 2.0 * math.cos(2.0 * math.pi * m * t)
    return total / beads


def split(v):
    hi = v.astype(BF16)
    lo = (v - hi.astype(F32)).astype(BF16)
    return hi, lo


def exact_dot(a, b):
    return jnp.dot(a, b, precision=HI, preferred_element_type=F32)


def fast_dot(a, b):
    return jnp.dot(a, b, preferred_element_type=F32)


def fast_dot_nt(a, b):
    return lax.dot_general(a, b, (((1,), (1,)), ((), ())), preferred_element_type=F32)


def kernel(
    nb, ns, own,
    pos_h, spc_h, nbr_h, cnt_h, snd_h, emb_h, wr_h, wm_h, wu_h, wo_h,
    out_ref,
    pos_v, spc_v, nbr_v, cnt_v, snd_v, emb_v, wr_v, wm_v, wu_v, wo_v,
    tx1, rx1,
    spc_r, snd_r, cnt_r, nbr_r, spc_l, snd_l, cnt_l, nbr_l, spc_rr, snd_rr, spc_ll, snd_ll,
    red_v, red_r, red_l, red_rr, red_ll,
    idx_v, idx_g, cnt_mat, cnt_gh, gb, ggb, cen, ceng, w1bc, wocol,
    p0r_hh, p0r_lo, p0_cat, wm_hh, wm_lo, wmt_hh, wmt_lo, wu_cat, wut_cat,
    h0_v, slope0, ah_v, al_v, z_v, zg_v, rinv_v, rinvg_v, x_v, q_v,
    dbs, fold_v, foldg_v, tx_r, tx_l, tx_rr, tx_ll, rx_r, rx_l, rx_rr, rx_ll, tx6, rx6,
    load_sem, s1, r1, sa, ra, s2, r2, s5, r5, s6, r6,
):
    beads, reduced = nb * own, nb
    scale = K ** -0.5
    b = lax.axis_index("bead")
    d = lax.axis_index("space")
    left = lax.rem(d + (ns - 1), ns)
    right = lax.rem(d + 1, ns)
    left2 = lax.rem(d + (ns - 2), ns)
    right2 = lax.rem(d + 2, ns)
    peers = [lax.rem(b + lag, nb) for lag in range(nb)]
    lags = by_distance(nb)

    def bead_copy(src, dst, ss, rs, lag):
        return pltpu.make_async_remote_copy(
            src_ref=src, dst_ref=dst, send_sem=ss, recv_sem=rs,
            device_id={"bead": peers[lag]}, device_id_type=MESH)

    def side_copy(src, dst, ss, rs, side):
        return pltpu.make_async_remote_copy(
            src_ref=src, dst_ref=dst, send_sem=ss, recv_sem=rs,
            device_id={"space": side}, device_id_type=MESH)

    barrier = pltpu.get_barrier_semaphore()
    for lag in lags:
        pl.semaphore_signal(barrier, inc=1, device_id={"bead": peers[lag]}, device_id_type=MESH)
    for side in (left, right, left2, right2):
        pl.semaphore_signal(barrier, inc=1, device_id={"space": side}, device_id_type=MESH)

    loads = []
    for i, (src, dst) in enumerate((
        (pos_h, pos_v), (spc_h, spc_v), (snd_h, snd_v), (nbr_h, nbr_v), (cnt_h, cnt_v),
        (emb_h, emb_v), (wr_h, wr_v), (wm_h, wm_v), (wu_h, wu_v), (wo_h, wo_v),
    )):
        copy = pltpu.make_async_copy(src, dst, load_sem.at[i])
        copy.start()
        loads.append(copy)

    loads[0].wait()
    packed = []
    for j in range(own):
        packed.append(jnp.concatenate(
            [pos_v[c, j : j + 1, half * H : half * H + H] for half in range(2) for c in range(3)], axis=0))
    for lag in range(nb):
        total = None
        for j in range(own):
            term = table_value(own * lag - j, beads, reduced) * packed[j]
            total = term if total is None else total + term
        tx1[lag] = total
    for copy in loads[1:5]:
        copy.wait()
    pl.semaphore_wait(barrier, nb + 3)

    first = {lag: bead_copy(tx1.at[lag], rx1.at[lag], s1.at[lag], r1.at[lag], lag) for lag in lags}
    for lag in lags:
        first[lag].start()
    near = pl.ds(0, H)
    far = pl.ds(H, H)
    aux = [
        side_copy(src, dst, sa.at[i], ra.at[i], side)
        for i, (src, dst, side) in enumerate((
            (nbr_v.at[:, near], nbr_r, left), (nbr_v.at[:, far], nbr_l, right),
            (cnt_v, cnt_r, left), (cnt_v, cnt_l, right),
            (spc_v, spc_r, left), (spc_v, spc_l, right), (spc_v, spc_rr, left2), (spc_v, spc_ll, right2),
            (snd_v, snd_r, left), (snd_v, snd_l, right), (snd_v, snd_rr, left2), (snd_v, snd_ll, right2),
        ))
    ]
    for copy in aux:
        copy.start()

    def rows_named(n, count):
        n = jnp.where(n >= A + G, n - G, jnp.where(n >= A, n + G, n))
        slot = lax.broadcasted_iota(jnp.int32, n.shape, 0)
        return jnp.where(slot < count, n, -1)

    def count_rows(idx, mat, width, rows):
        def step(i, carry):
            base = pl.multiple_of(i * rows, rows)
            row = lax.broadcasted_iota(jnp.int32, (rows, width), 0) + base
            acc = jnp.zeros((rows, width), F32)
            for k in range(K):
                acc = acc + jnp.where(idx[k : k + 1, :] == row, 1.0, 0.0)
            mat[pl.ds(base, rows), :] = acc
            return carry

        lax.fori_loop(0, E // rows, step, 0)

    idx_v[...] = rows_named(nbr_v[...], jnp.concatenate([cnt_v[0:1, :], cnt_v[1:2, :]], axis=1))
    count_rows(idx_v, cnt_mat, A, 32)

    for copy in loads[5:]:
        copy.wait()
    zeros6 = jnp.zeros((6, CH), F32)
    emb8 = jnp.concatenate([emb_v[...], zeros6], axis=0)
    table = exact_dot(emb8, wm_v[0])
    w0 = wr_v[0] * scale
    rows0 = jnp.concatenate([w0 * table[0:1], w0 * (table[1:2] - table[0:1])], axis=0)
    p0 = exact_dot(rows0, wu_v[0])
    p0_hi, p0_lo = split(p0)
    p0_cat[...] = jnp.concatenate([p0_hi, p0_lo], axis=1)
    hi, lo = split(jnp.concatenate(
        [jnp.broadcast_to(p0[j : j + 1, :], (8, CH)) for j in range(2 * NB)], axis=0))
    p0r_hh[...] = jnp.concatenate([hi, hi], axis=0)
    p0r_lo[...] = lo
    w1 = wr_v[1] * scale
    w1t = jnp.transpose(jnp.concatenate([w1, jnp.zeros((CH - NB, CH), F32)], axis=0))
    for k in range(NB):
        w1bc[k] = jnp.broadcast_to(w1t[:, k : k + 1], (CH, H))
    hi, lo = split(wm_v[1])
    wm_hh[...] = jnp.concatenate([hi, hi], axis=0)
    wm_lo[...] = lo
    hi, lo = split(jnp.transpose(wm_v[1]))
    wmt_hh[...] = jnp.concatenate([hi, hi], axis=0)
    wmt_lo[...] = lo
    hi, lo = split(wu_v[1])
    wu_cat[...] = jnp.concatenate([hi, lo], axis=1)
    hi, lo = split(jnp.transpose(wu_v[1]))
    wut_cat[...] = jnp.concatenate([hi, lo], axis=1)
    wocol[...] = jnp.transpose(jnp.broadcast_to(wo_v[...], (CH, CH)))

    lane = lax.broadcasted_iota(jnp.int32, (1, H), 1)
    low = lane < G

    red = tx1[0]
    for lag in lags:
        first[lag].wait_recv()
        red = red + rx1[lag]
    red_v[...] = red
    second = [
        side_copy(red_v, dst, s2.at[i], r2.at[i], side)
        for i, (dst, side) in enumerate(((red_r, left), (red_l, right), (red_rr, left2), (red_ll, right2)))
    ]
    for copy in second:
        copy.start()

    for copy in aux:
        copy.wait_recv()
    idx_g[...] = rows_named(
        jnp.where(low, nbr_r[...], nbr_l[...]), jnp.where(low, cnt_r[0:1, :], cnt_l[1:2, :]))
    count_rows(idx_g, cnt_gh, H, 64)
    natural = lax.broadcasted_iota(jnp.int32, (H, H), 0)

    def reorder(from_right, from_left, rows):
        order = jnp.where(low, from_right, from_left - (A - H))
        return fast_dot(jnp.where(natural == order, 1.0, 0.0).astype(BF16), rows)

    cnt_mat[pl.ds(A, 2 * G), :] = reorder(snd_r[...], snd_l[...], cnt_mat[pl.ds(A, 2 * G), :].astype(BF16))
    rows_gh = cnt_gh[pl.ds(A, 2 * G), :].astype(BF16)
    cnt_gh[pl.ds(A, 2 * G), :] = jnp.where(
        low, reorder(snd_rr[...], snd_v[...], rows_gh), reorder(snd_v[...], snd_ll[...], rows_gh))
    kind_own = spc_v[...].astype(F32)
    kind_r, kind_l = spc_r[...].astype(F32), spc_l[...].astype(F32)
    kind_gh = jnp.where(low, kind_r[0:1], kind_l[1:2])
    kind_rg = jnp.where(low, spc_rr[0:1, :].astype(F32), kind_own[1:2])
    kind_lg = jnp.where(low, kind_own[0:1], spc_ll[1:2, :].astype(F32))
    zrest = jnp.zeros((CH - 4, H), F32)
    z3 = jnp.zeros((3, H), F32)
    for part, kind in enumerate((kind_own[0:1], kind_own[1:2], kind_gh)):
        kcol = jnp.transpose(jnp.concatenate([z3, kind, zrest], axis=0))
        h0_v[pl.ds(part * H, H), :] = jnp.where(kcol[:, 3:4] > 0.5, emb_v[1:2, :], emb_v[0:1, :])
    cen[...] = jnp.concatenate(
        [jnp.concatenate([red[0:3], red[3:6]], axis=1), jnp.zeros((5, A), F32)], axis=0)

    def spread_rows(part, pieces):
        col = jnp.transpose(jnp.concatenate(pieces + [zrest], axis=0))
        for c in range(4):
            gb[c, pl.ds(part * H, H), :] = jnp.broadcast_to(col[:, c : c + 1], (H, H))

    for half in range(2):
        spread_rows(half, [red[3 * half : 3 * half + 3], kind_own[half : half + 1]])

    def folded(v):
        total = v[0:8]
        for r in range(8, v.shape[0], 8):
            total = total + v[r : r + 8]
        return total

    def pair_rows(start):
        rows = 16

        def step(i, carry):
            base = pl.multiple_of(start + i * rows, rows)
            at = pl.ds(base, rows)
            gx, gy, gz, kind = [gb[c, at, :] for c in range(4)]
            sums = list(carry)
            for half in range(2):
                lanes = pl.ds(half * H, H)
                dx, dy, dz = gx - cen[0:1, lanes], gy - cen[1:2, lanes], gz - cen[2:3, lanes]
                square = dx * dx + dy * dy + dz * dz + FLOOR
                rinv = lax.rsqrt(square)
                x = square * rinv * STEP
                rinv_v[at, lanes] = rinv
                c = cnt_mat[at, lanes]
                for k in range(NB):
                    off = x - CENTERS[k]
                    a = c * jnp.exp2(-(off * off))
                    hi, lo = split(a)
                    ah_v[pl.ds(k * E + base, rows), lanes] = hi
                    al_v[pl.ds(k * E + base, rows), lanes] = lo
                    z_v[pl.ds(k * E + base, rows), lanes] = a * off
                    sums[2 * k + half] = sums[2 * k + half] + folded(a)
                    j = 2 * NB + 2 * k + half
                    sums[j] = sums[j] + folded(a * kind)
            return tuple(sums)

        return step

    sums = tuple(jnp.zeros((8, H), F32) for _ in range(4 * NB))
    sums = lax.fori_loop(0, A // 16, pair_rows(0), sums, unroll=UNROLL)
    for copy in second:
        copy.wait_recv()

    def shifted(at_left, at_right, values):
        shift = jnp.where(low, jnp.where(at_right, float(ns), 0.0), jnp.where(at_left, -float(ns), 0.0))
        first_row = lax.broadcasted_iota(jnp.int32, (3, H), 0) == 0
        return values + jnp.where(first_row, shift, 0.0)

    borrowed = jnp.where(low, red_r[0:3, :], red_l[3:6, :])
    ceng[...] = jnp.concatenate([borrowed, jnp.zeros((5, H), F32)], axis=0)
    ghost = shifted(d == 0, d == ns - 1, borrowed)
    ghost_r = shifted(right == 0, right == ns - 1, jnp.where(low, red_rr[0:3, :], red[3:6]))
    ghost_l = shifted(left == 0, left == ns - 1, jnp.where(low, red[0:3], red_ll[3:6, :]))
    spread_rows(2, [ghost, kind_gh])
    zrest8 = jnp.zeros((CH - 8, H), F32)
    for part, pieces in enumerate((
        (red_r[0:3, :], kind_r[0:1], red_l[0:3, :], kind_l[0:1]),
        (red_r[3:6, :], kind_r[1:2], red_l[3:6, :], kind_l[1:2]),
        (ghost_r, kind_rg, ghost_l, kind_lg),
    )):
        col = jnp.transpose(jnp.concatenate(list(pieces) + [zrest8], axis=0))
        for c in range(4):
            ggb[c, pl.ds(part * H, H), :] = jnp.where(low, col[:, c : c + 1], col[:, c + 4 : c + 5])

    def ghost_rows(i, carry):
        rows = 32
        base = pl.multiple_of(i * rows, rows)
        dx, dy, dz = [ggb[c, pl.ds(base, rows), :] - ceng[c : c + 1, :] for c in range(3)]
        kind = ggb[3, pl.ds(base, rows), :]
        square = dx * dx + dy * dy + dz * dz + FLOOR
        rinv = lax.rsqrt(square)
        x = square * rinv * STEP
        rinvg_v[pl.ds(base, rows), :] = rinv
        c = cnt_gh[pl.ds(base, rows), :]
        sums = list(carry)
        for k in range(NB):
            off = x - CENTERS[k]
            a = c * jnp.exp2(-(off * off))
            zg_v[pl.ds(k * E + base, rows), :] = a * off
            s = a * kind
            sums[k] = sums[k] + folded(a)
            sums[NB + k] = sums[NB + k] + folded(s)
        return tuple(sums)

    sums = lax.fori_loop(0, 2 * G // 16, pair_rows(A), sums, unroll=UNROLL)
    gsums = tuple(jnp.zeros((8, H), F32) for _ in range(2 * NB))
    gsums = lax.fori_loop(0, E // 32, ghost_rows, gsums, unroll=UNROLL)

    stacked = jnp.concatenate(
        [jnp.concatenate(sums[0::2], axis=0), jnp.concatenate(sums[1::2], axis=0),
         jnp.concatenate(gsums, axis=0)], axis=1)
    hi, lo = split(jnp.transpose(stacked))
    u0 = fast_dot(jnp.concatenate([hi, lo], axis=1), p0r_hh[...]) + fast_dot(hi, p0r_lo[...])
    sig0 = 1.0 / (1.0 + jnp.exp(-u0))
    slope0[...] = sig0 * (1.0 + u0 * (1.0 - sig0))
    hi, lo = split(h0_v[...] + u0 * sig0)
    lent = fast_dot(jnp.concatenate([hi, lo], axis=1), wm_hh[...]) + fast_dot(hi, wm_lo[...])

    lt = jnp.transpose(lent)
    for k in range(NB):
        w = w1bc[k]
        hi, lo = split(lt * jnp.concatenate([w, w, w], axis=1))
        x_v[pl.ds(0, CH), pl.ds(k * E, E)] = hi
        x_v[pl.ds(CH, CH), pl.ds(k * E, E)] = lo
    both = fast_dot(x_v[...], ah_v[...])
    message = both[:CH] + both[CH:] + fast_dot(x_v[pl.ds(0, CH), :], al_v[...])
    hi, lo = split(message)
    wut = wut_cat[...]
    u1 = fast_dot(wut, jnp.concatenate([hi, hi], axis=0)) + fast_dot(wut[:, :CH], lo)
    sig1 = 1.0 / (1.0 + jnp.exp(-u1))
    wo2 = jnp.concatenate([wocol[...], wocol[...]], axis=1)
    hi, lo = split(wo2 * (sig1 * (1.0 + u1 * (1.0 - sig1))))
    wu = wu_cat[...]
    gm1t = fast_dot(wu, jnp.concatenate([hi, hi], axis=0)) + fast_dot(wu[:, :CH], lo)
    gm_hi, gm_lo = split(jnp.transpose(gm1t))
    gcat = jnp.concatenate([gm_hi, gm_lo], axis=1)
    dl = None
    for k in range(NB):
        y = fast_dot(ah_v[pl.ds(k * E, E), :], gcat)
        y2 = fast_dot(al_v[pl.ds(k * E, E), :], gm_hi)
        term = w1[k : k + 1, :] * (y[:, :CH] + y[:, CH:] + y2)
        dl = term if dl is None else dl + term
    hi, lo = split(dl)
    gh1 = fast_dot(jnp.concatenate([hi, lo], axis=1), wmt_hh[...]) + fast_dot(hi, wmt_lo[...])
    gh1 = jnp.concatenate([gh1[:A] + wo_v[...], gh1[A:]], axis=0)
    hi, lo = split(gh1 * slope0[...])
    p0c = p0_cat[...]
    db = fast_dot_nt(p0c, jnp.concatenate([hi, hi], axis=1)) + fast_dot_nt(p0c[:, :CH], lo)
    dbs[...] = jnp.concatenate([db[0:NB], db[0:NB] + db[NB : 2 * NB]], axis=0)
    l_hi, l_lo = split(lent)
    lcat = jnp.concatenate([l_hi, l_lo], axis=1)
    for k in range(NB):
        w = w1bc[k]
        hi, lo = split(gm1t * jnp.concatenate([w, w], axis=1))
        da = fast_dot(lcat, jnp.concatenate([hi, hi], axis=0)) + fast_dot(l_hi, lo)
        term = da * z_v[pl.ds(k * E, E), :]
        q_v[...] = term if k == 0 else q_v[...] + term

    factor = -2.0 / (0.2 * ROOT)

    def force_rows(start):
        rows = 16

        def step(i, carry):
            base = pl.multiple_of(start + i * rows, rows)
            at = pl.ds(base, rows)
            kind = gb[3, at, :] > 0.5
            new = list(carry)
            folds = [None] * 3
            for half in range(2):
                lanes = pl.ds(half * H, H)
                q = q_v[at, lanes]
                for k in range(NB):
                    coef = jnp.where(kind, dbs[NB + k : NB + k + 1, lanes], dbs[k : k + 1, lanes])
                    q = q + coef * z_v[pl.ds(k * E + base, rows), lanes]
                g = q * rinv_v[at, lanes] * factor
                for c in range(3):
                    f = g * (gb[c, at, :] - cen[c : c + 1, lanes])
                    folds[c] = f if half == 0 else folds[c] + f
                    new[2 * c + half] = new[2 * c + half] + folded(f)
            for c in range(3):
                fold_v[c, at, :] = folds[c]
            return tuple(new)

        return step

    def ghost_force(i, carry):
        rows = 32
        base = pl.multiple_of(i * rows, rows)
        kind = ggb[3, pl.ds(base, rows), :] > 0.5
        q = None
        for k in range(NB):
            coef = jnp.where(kind, dbs[NB + k : NB + k + 1, A:], dbs[k : k + 1, A:])
            term = coef * zg_v[pl.ds(k * E + base, rows), :]
            q = term if q is None else q + term
        g = q * rinvg_v[pl.ds(base, rows), :] * factor
        new = []
        for c in range(3):
            f = g * (ggb[c, pl.ds(base, rows), :] - ceng[c : c + 1, :])
            foldg_v[c, pl.ds(base, rows), :] = f
            new.append(carry[c] + folded(f))
        return tuple(new)

    def row_sums(start):
        return jnp.concatenate(
            [jnp.sum(jnp.transpose(fold_v[c, pl.ds(start, H), :]), axis=0, keepdims=True)
             for c in range(3)], axis=0)

    def ghost_sums(start):
        turned = [jnp.transpose(foldg_v[c, pl.ds(start, H), :]) for c in range(3)]
        return [
            jnp.concatenate([jnp.sum(t[G * part : G * part + G], axis=0, keepdims=True) for t in turned], axis=0)
            for part in range(2)
        ]

    gpulls = tuple(jnp.zeros((8, H), F32) for _ in range(3))
    gpulls = lax.fori_loop(0, E // 32, ghost_force, gpulls, unroll=UNROLL)
    pulls = tuple(jnp.zeros((8, H), F32) for _ in range(6))
    pulls = lax.fori_loop(0, 2 * G // 16, force_rows(A), pulls, unroll=UNROLL)
    lent_pull = row_sums(A) - jnp.concatenate([jnp.sum(v, axis=0, keepdims=True) for v in gpulls], axis=0)
    r_low, l_low = ghost_sums(0)
    r_high, l_high = ghost_sums(H)
    r_end, l_end = ghost_sums(2 * H)
    tx_r[...] = jnp.concatenate([r_low + jnp.where(low, lent_pull, 0.0), r_high], axis=0)
    tx_l[...] = jnp.concatenate([l_low, l_high + jnp.where(low, 0.0, lent_pull)], axis=0)
    tx_rr[...] = r_end
    tx_ll[...] = l_end
    fifth = [
        side_copy(src, dst, s5.at[i], r5.at[i], side)
        for i, (src, dst, side) in enumerate((
            (tx_r, rx_l, right), (tx_l, rx_r, left), (tx_rr, rx_ll, right2), (tx_ll, rx_rr, left2)))
    ]
    for copy in fifth:
        copy.start()
    pulls = lax.fori_loop(0, A // 16, force_rows(0), pulls, unroll=UNROLL)
    centre = [jnp.sum(v, axis=0, keepdims=True) for v in pulls]
    lower = jnp.concatenate(centre[0::2], axis=0) - row_sums(0) - jnp.where(low, l_end, 0.0)
    upper = jnp.concatenate(centre[1::2], axis=0) - row_sums(H) - jnp.where(low, 0.0, r_end)
    for copy in fifth:
        copy.wait_recv()
    lower = lower - jnp.where(low, rx_ll[...], 0.0)
    upper = upper - jnp.where(low, 0.0, rx_rr[...])
    pull = jnp.concatenate([lower, upper], axis=0) - (rx_l[...] + rx_r[...])
    tx6[...] = pull
    last = {lag: bead_copy(tx6, rx6.at[lag], s6.at[lag], r6.at[lag], lag) for lag in lags}
    for lag in lags:
        last[lag].start()
    ratio = beads / reduced
    totals = [ratio * table_value(-j, beads, reduced) * pull for j in range(own)]
    for lag in reversed(lags):
        last[lag].wait_recv()
        arrived = rx6[lag]
        for j in range(own):
            totals[j] = totals[j] + ratio * table_value(-own * lag - j, beads, reduced) * arrived
    for c in range(3):
        for half in range(2):
            row = 3 * half + c
            out_ref[c, :, half * H : half * H + H] = jnp.concatenate(
                [totals[j][row : row + 1] for j in range(own)], axis=0)
    for copy in list(first.values()) + aux + second + fifth + list(last.values()):
        copy.wait_send()


def solution(mesh):
    nb, ns = mesh.shape["bead"], mesh.shape["space"]

    def on_device(positions, species, neighbors, counts, send_rows, embed, w_radial, w_msg, w_upd, w_out):
        own = positions.shape[0]
        dma = pltpu.SemaphoreType.DMA

        def f32(*dims):
            return pltpu.VMEM(dims, F32)

        def i32(*dims):
            return pltpu.VMEM(dims, jnp.int32)

        def b16(*dims):
            return pltpu.VMEM(dims, BF16)

        scratch = [
            f32(3, own, A), i32(2, H), i32(K, A), i32(2, H), i32(1, H), f32(2, CH), f32(2, NB, CH),
            f32(2, CH, CH), f32(2, CH, CH), f32(1, CH),
            f32(nb, 6, H), f32(nb, 6, H),
            i32(2, H), i32(1, H), i32(2, H), i32(K, H), i32(2, H), i32(1, H), i32(2, H), i32(K, H),
            i32(2, H), i32(1, H), i32(2, H), i32(1, H),
            f32(6, H), f32(6, H), f32(6, H), f32(6, H), f32(6, H),
            i32(K, A), i32(K, H), f32(E, A), f32(E, H), f32(4, E, H), f32(4, E, H), f32(8, A), f32(8, H),
            f32(NB, CH, H), f32(CH, CH),
            b16(2 * CH, CH), b16(CH, CH), b16(2 * NB, 2 * CH), b16(2 * CH, CH), b16(CH, CH),
            b16(2 * CH, CH), b16(CH, CH), b16(CH, 2 * CH), b16(CH, 2 * CH),
            f32(E, CH), f32(E, CH), b16(NB * E, A), b16(NB * E, A), f32(NB * E, A), f32(NB * E, H),
            f32(E, A), f32(E, H), b16(2 * CH, NB * E), f32(E, A),
            f32(2 * NB, E), f32(3, E, H), f32(3, E, H),
            f32(6, H), f32(6, H), f32(3, H), f32(3, H), f32(6, H), f32(6, H), f32(3, H), f32(3, H),
            f32(6, H), f32(nb, 6, H),
            dma((10,)), dma((nb,)), dma((nb,)), dma((12,)), dma((12,)), dma((4,)), dma((4,)), dma((4,)), dma((4,)),
            dma((nb,)), dma((nb,)),
        ]
        forces = pl.pallas_call(
            functools.partial(kernel, nb, ns, own),
            out_shape=jax.ShapeDtypeStruct((3, own, A), F32),
            in_specs=[pl.BlockSpec(memory_space=pltpu.HBM)] * 10,
            out_specs=pl.BlockSpec(memory_space=pltpu.VMEM),
            scratch_shapes=scratch,
            compiler_params=pltpu.CompilerParams(
                collective_id=0, has_side_effects=True, vmem_limit_bytes=40 * 1024 * 1024),
        )(
            *[pltpu.with_memory_space_constraint(v, pltpu.HBM) for v in (positions.transpose(1, 0, 2), species.reshape(2, H), neighbors, counts.reshape(2, H),
            send_rows.reshape(1, H), embed, w_radial, w_msg, w_upd, w_out.reshape(1, CH))],
        )
        return forces.transpose(1, 0, 2)

    return jax.shard_map(
        on_device,
        mesh=mesh,
        in_specs=(
            P("bead", None, "space"), P("space"), P(None, "space"), P("space"), P("space"),
            P(), P(), P(), P(), P(),
        ),
        out_specs=P("bead", None, "space"),
        check_vma=False,
    )
```

```python
import functools
import math

import jax
import jax.numpy as jnp
from jax import lax
from jax.experimental import pallas as pl
from jax.experimental.pallas import tpu as pltpu
from jax.sharding import PartitionSpec as P

MESH = pl.DeviceIdType.MESH
HI = lax.Precision.HIGHEST
F32 = jnp.float32
BF16 = jnp.bfloat16

NB = 8
CH = 128
A = 256
G = 64
E = A + 2 * G
K = 32
H = 128
ROOT = math.sqrt(math.log2(math.e))
STEP = ROOT / 0.2
CENTERS = tuple(STEP * 1.5 * b / (NB - 1) for b in range(NB))
FLOOR = 0.01
UNROLL = 2


def by_distance(nb):
    def far(lag):
        dz, dx = lag % 4, lag // 4
        return -(2 * min(dz, 4 - dz) + min(dx, 4 - dx))

    return sorted(range(1, nb), key=far)


def table_value(lag, beads, reduced):
    t = lag / beads
    total = 1.0 + math.cos(math.pi * reduced * t)
    for m in range(1, reduced // 2):
        total += 2.0 * math.cos(2.0 * math.pi * m * t)
    return total / beads


def split(v):
    hi = v.astype(BF16)
    lo = (v - hi.astype(F32)).astype(BF16)
    return hi, lo


def exact_dot(a, b):
    return jnp.dot(a, b, precision=HI, preferred_element_type=F32)


def fast_dot(a, b):
    return jnp.dot(a, b, preferred_element_type=F32)


def wide(w):
    hi, lo = split(w)
    row = jnp.concatenate([hi, lo], axis=1)
    return jnp.concatenate([row, row], axis=0)


def wide_dot(a, w):
    hi, lo = split(a)
    both = fast_dot(jnp.concatenate([hi, lo], axis=1), w)
    return both[:, :CH] + both[:, CH:]


def fast_dot_nt(a, b):
    return lax.dot_general(a, b, (((1,), (1,)), ((), ())), preferred_element_type=F32)


def kernel(
    nb, ns, own,
    pos_h, spc_h, nbr_h, cnt_h, snd_h, emb_h, wr_h, wm_h, wu_h, wo_h,
    out_ref,
    pos_v, spc_v, nbr_v, cnt_v, snd_v, emb_v, wr_v, wm_v, wu_v, wo_v,
    tx1, rx1,
    spc_r, snd_r, cnt_r, nbr_r, spc_l, snd_l, cnt_l, nbr_l, spc_rr, snd_rr, spc_ll, snd_ll,
    red_v, red_r, red_l, red_rr, red_ll,
    idx_v, idx_g, cnt_mat, cnt_gh, gb, ggb, cen, ceng, w1bc, wocol,
    p0r_w, p0_cat, wm_w, wmt_w, wu_cat, wut_cat,
    h0_v, slope0, ah_v, al_v, z_v, zg_v, rinv_v, rinvg_v, gs_v, q_v,
    pick_v, dbs, fold_v, foldg_v, tx_r, tx_l, tx_rr, tx_ll, rx_r, rx_l, rx_rr, rx_ll, tx6, rx6,
    load_sem, s1, r1, sa, ra, s2, r2, s5, r5, s6, r6,
):
    beads, reduced = nb * own, nb
    scale = K ** -0.5
    b = lax.axis_index("bead")
    d = lax.axis_index("space")
    left = lax.rem(d + (ns - 1), ns)
    right = lax.rem(d + 1, ns)
    left2 = lax.rem(d + (ns - 2), ns)
    right2 = lax.rem(d + 2, ns)
    peers = [lax.rem(b + lag, nb) for lag in range(nb)]
    lags = by_distance(nb)

    def bead_copy(src, dst, ss, rs, lag):
        return pltpu.make_async_remote_copy(
            src_ref=src, dst_ref=dst, send_sem=ss, recv_sem=rs,
            device_id=peers[lag] * ns + d, device_id_type=pl.DeviceIdType.LOGICAL)

    def side_copy(src, dst, ss, rs, side):
        return pltpu.make_async_remote_copy(
            src_ref=src, dst_ref=dst, send_sem=ss, recv_sem=rs,
            device_id=b * ns + side, device_id_type=pl.DeviceIdType.LOGICAL)

    barrier = pltpu.get_barrier_semaphore()
    for lag in lags:
        pl.semaphore_signal(barrier, inc=1, device_id=peers[lag] * ns + d, device_id_type=pl.DeviceIdType.LOGICAL)
    for side in (left, right, left2, right2):
        pl.semaphore_signal(barrier, inc=1, device_id=b * ns + side, device_id_type=pl.DeviceIdType.LOGICAL)

    loads = []
    for i, (src, dst) in enumerate((
        (pos_h, pos_v), (spc_h, spc_v), (snd_h, snd_v), (nbr_h, nbr_v), (cnt_h, cnt_v),
        (emb_h, emb_v), (wr_h, wr_v), (wm_h, wm_v), (wu_h, wu_v), (wo_h, wo_v),
    )):
        copy = pltpu.make_async_copy(src, dst, load_sem.at[i])
        copy.start()
        loads.append(copy)

    loads[0].wait()
    packed = []
    for j in range(own):
        packed.append(jnp.concatenate(
            [pos_v[c, j : j + 1, half * H : half * H + H] for half in range(2) for c in range(3)], axis=0))
    for lag in range(nb):
        total = None
        for j in range(own):
            term = table_value(own * lag - j, beads, reduced) * packed[j]
            total = term if total is None else total + term
        tx1[lag] = total
    for copy in loads[1:5]:
        copy.wait()
    pl.semaphore_wait(barrier, nb + 3)

    first = {lag: bead_copy(tx1.at[lag], rx1.at[lag], s1.at[lag], r1.at[lag], lag) for lag in lags}
    for lag in lags:
        first[lag].start()
    near = pl.ds(0, H)
    far = pl.ds(H, H)
    aux = [
        side_copy(src, dst, sa.at[i], ra.at[i], side)
        for i, (src, dst, side) in enumerate((
            (nbr_v.at[:, near], nbr_r, left), (nbr_v.at[:, far], nbr_l, right),
            (cnt_v, cnt_r, left), (cnt_v, cnt_l, right),
            (spc_v, spc_r, left), (spc_v, spc_l, right), (spc_v, spc_rr, left2), (spc_v, spc_ll, right2),
            (snd_v, snd_r, left), (snd_v, snd_l, right), (snd_v, snd_rr, left2), (snd_v, snd_ll, right2),
        ))
    ]
    for copy in aux:
        copy.start()

    def rows_named(n, count):
        n = jnp.where(n >= A + G, n - G, jnp.where(n >= A, n + G, n))
        slot = lax.broadcasted_iota(jnp.int32, n.shape, 0)
        return jnp.where(slot < count, n, -1)

    def count_rows(idx, mat, width, rows):
        def step(i, carry):
            base = pl.multiple_of(i * rows, rows)
            row = lax.broadcasted_iota(jnp.int32, (rows, width), 0) + base
            acc = jnp.zeros((rows, width), F32)
            for k in range(K):
                acc = acc + jnp.where(idx[k : k + 1, :] == row, 1.0, 0.0)
            mat[pl.ds(base, rows), :] = acc
            return carry

        lax.fori_loop(0, E // rows, step, 0)

    idx_v[...] = rows_named(nbr_v[...], jnp.concatenate([cnt_v[0:1, :], cnt_v[1:2, :]], axis=1))
    count_rows(idx_v, cnt_mat, A, 32)

    for copy in loads[5:]:
        copy.wait()
    zeros6 = jnp.zeros((6, CH), F32)
    emb8 = jnp.concatenate([emb_v[...], zeros6], axis=0)
    table = exact_dot(emb8, wm_v[0])
    w0 = wr_v[0] * scale
    rows0 = jnp.concatenate([w0 * table[0:1], w0 * (table[1:2] - table[0:1])], axis=0)
    p0 = exact_dot(rows0, wu_v[0])
    p0_hi, p0_lo = split(p0)
    p0_cat[...] = jnp.concatenate([p0_hi, p0_lo], axis=1)
    p0r_w[...] = wide(jnp.concatenate(
        [jnp.broadcast_to(p0[j : j + 1, :], (8, CH)) for j in range(2 * NB)], axis=0))
    w1 = wr_v[1] * scale
    w1t = jnp.transpose(jnp.concatenate([w1, jnp.zeros((CH - NB, CH), F32)], axis=0))
    for k in range(NB):
        w1bc[k] = jnp.broadcast_to(w1t[:, k : k + 1], (CH, H))
    wm_w[...] = wide(wm_v[1])
    wmt_w[...] = wide(jnp.transpose(wm_v[1]))
    hi, lo = split(wu_v[1])
    wu_cat[...] = jnp.concatenate([hi, lo], axis=1)
    hi, lo = split(jnp.transpose(wu_v[1]))
    wut_cat[...] = jnp.concatenate([hi, lo], axis=1)
    wocol[...] = jnp.transpose(jnp.broadcast_to(wo_v[...], (CH, CH)))

    lane = lax.broadcasted_iota(jnp.int32, (1, H), 1)
    low = lane < G

    row = lax.broadcasted_iota(jnp.int32, (CH, 4 * H), 0)
    spot = lax.broadcasted_iota(jnp.int32, (CH, 4 * H), 1)
    value = spot // H + jnp.where(spot % H < G, 0, 4)
    pick_v[...] = jnp.where((row < 24) & (row % 8 == value), 1.0, 0.0).astype(BF16)

    red = tx1[0]
    for lag in lags:
        first[lag].wait_recv()
        red = red + rx1[lag]
    red_v[...] = red
    second = [
        side_copy(red_v, dst, s2.at[i], r2.at[i], side)
        for i, (dst, side) in enumerate(((red_r, left), (red_l, right), (red_rr, left2), (red_ll, right2)))
    ]
    for copy in second:
        copy.start()

    for copy in aux:
        copy.wait_recv()
    idx_g[...] = rows_named(
        jnp.where(low, nbr_r[...], nbr_l[...]), jnp.where(low, cnt_r[0:1, :], cnt_l[1:2, :]))
    count_rows(idx_g, cnt_gh, H, 64)
    natural = lax.broadcasted_iota(jnp.int32, (H, H), 0)

    def reorder(from_right, from_left, rows):
        order = jnp.where(low, from_right, from_left - (A - H))
        return fast_dot(jnp.where(natural == order, 1.0, 0.0).astype(BF16), rows)

    cnt_mat[pl.ds(A, 2 * G), :] = reorder(snd_r[...], snd_l[...], cnt_mat[pl.ds(A, 2 * G), :].astype(BF16))
    rows_gh = cnt_gh[pl.ds(A, 2 * G), :].astype(BF16)
    cnt_gh[pl.ds(A, 2 * G), :] = jnp.where(
        low, reorder(snd_rr[...], snd_v[...], rows_gh), reorder(snd_v[...], snd_ll[...], rows_gh))
    kind_own = spc_v[...].astype(F32)
    kind_r, kind_l = spc_r[...].astype(F32), spc_l[...].astype(F32)
    kind_gh = jnp.where(low, kind_r[0:1], kind_l[1:2])
    kind_rg = jnp.where(low, spc_rr[0:1, :].astype(F32), kind_own[1:2])
    kind_lg = jnp.where(low, kind_own[0:1], spc_ll[1:2, :].astype(F32))
    zrest = jnp.zeros((CH - 4, H), F32)
    z3 = jnp.zeros((3, H), F32)
    for part, kind in enumerate((kind_own[0:1], kind_own[1:2], kind_gh)):
        kcol = jnp.transpose(jnp.concatenate([z3, kind, zrest], axis=0))
        h0_v[pl.ds(part * H, H), :] = jnp.where(kcol[:, 3:4] > 0.5, emb_v[1:2, :], emb_v[0:1, :])
    cen[...] = jnp.concatenate(
        [jnp.concatenate([red[0:3], red[3:6]], axis=1), jnp.zeros((5, A), F32)], axis=0)

    def spread_rows(part, pieces):
        col = jnp.transpose(jnp.concatenate(pieces + [zrest], axis=0))
        for c in range(4):
            gb[c, pl.ds(part * H, H), :] = jnp.broadcast_to(col[:, c : c + 1], (H, H))

    for half in range(2):
        spread_rows(half, [red[3 * half : 3 * half + 3], kind_own[half : half + 1]])

    def folded(v):
        total = v[0:8]
        for r in range(8, v.shape[0], 8):
            total = total + v[r : r + 8]
        return total

    def pair_rows(start):
        rows = 16

        def step(i, carry):
            base = pl.multiple_of(start + i * rows, rows)
            at = pl.ds(base, rows)
            gx, gy, gz, kind = [gb[c, at, :] for c in range(4)]
            sums = list(carry)
            for half in range(2):
                lanes = pl.ds(half * H, H)
                dx, dy, dz = gx - cen[0:1, lanes], gy - cen[1:2, lanes], gz - cen[2:3, lanes]
                square = dx * dx + dy * dy + dz * dz + FLOOR
                rinv = lax.rsqrt(square)
                x = square * rinv * STEP
                rinv_v[at, lanes] = rinv
                c = cnt_mat[at, lanes]
                for k in range(NB):
                    off = x - CENTERS[k]
                    a = c * jnp.exp2(-(off * off))
                    hi, lo = split(a)
                    spot = pl.ds(k * A + half * H, H)
                    ah_v[at, spot] = hi
                    al_v[at, spot] = lo
                    z_v[pl.ds(k * E + base, rows), lanes] = a * off
                    sums[2 * k + half] = sums[2 * k + half] + folded(a)
                    j = 2 * NB + 2 * k + half
                    sums[j] = sums[j] + folded(a * kind)
            return tuple(sums)

        return step

    sums = tuple(jnp.zeros((8, H), F32) for _ in range(4 * NB))
    sums = lax.fori_loop(0, A // 16, pair_rows(0), sums, unroll=UNROLL)
    for copy in second:
        copy.wait_recv()

    def shifted(at_left, at_right, values):
        shift = jnp.where(low, jnp.where(at_right, float(ns), 0.0), jnp.where(at_left, -float(ns), 0.0))
        first_row = lax.broadcasted_iota(jnp.int32, (3, H), 0) == 0
        return values + jnp.where(first_row, shift, 0.0)

    borrowed = jnp.where(low, red_r[0:3, :], red_l[3:6, :])
    ceng[...] = jnp.concatenate([borrowed, jnp.zeros((5, H), F32)], axis=0)
    ghost = shifted(d == 0, d == ns - 1, borrowed)
    ghost_r = shifted(right == 0, right == ns - 1, jnp.where(low, red_rr[0:3, :], red[3:6]))
    ghost_l = shifted(left == 0, left == ns - 1, jnp.where(low, red[0:3], red_ll[3:6, :]))
    spread_rows(2, [ghost, kind_gh])
    for part, pieces in enumerate((
        (red_r[0:3, :], kind_r[0:1], red_l[0:3, :], kind_l[0:1]),
        (red_r[3:6, :], kind_r[1:2], red_l[3:6, :], kind_l[1:2]),
        (ghost_r, kind_rg, ghost_l, kind_lg),
    )):
        rest = jnp.concatenate(list(pieces), axis=0)
        layers = []
        for _ in range(3):
            layer = rest.astype(BF16).astype(F32)
            layers.append(layer)
            rest = rest - layer
        col = jnp.transpose(jnp.concatenate(layers + [jnp.zeros((CH - 24, H), F32)], axis=0)).astype(BF16)
        spread = fast_dot(col, pick_v[...])
        for c in range(4):
            ggb[c, pl.ds(part * H, H), :] = spread[:, c * H : c * H + H]

    def ghost_rows(i, carry):
        rows = 32
        base = pl.multiple_of(i * rows, rows)
        dx, dy, dz = [ggb[c, pl.ds(base, rows), :] - ceng[c : c + 1, :] for c in range(3)]
        kind = ggb[3, pl.ds(base, rows), :]
        square = dx * dx + dy * dy + dz * dz + FLOOR
        rinv = lax.rsqrt(square)
        x = square * rinv * STEP
        rinvg_v[pl.ds(base, rows), :] = rinv
        c = cnt_gh[pl.ds(base, rows), :]
        sums = list(carry)
        for k in range(NB):
            off = x - CENTERS[k]
            a = c * jnp.exp2(-(off * off))
            zg_v[pl.ds(k * E + base, rows), :] = a * off
            s = a * kind
            sums[k] = sums[k] + folded(a)
            sums[NB + k] = sums[NB + k] + folded(s)
        return tuple(sums)

    sums = lax.fori_loop(0, 2 * G // 16, pair_rows(A), sums, unroll=UNROLL)
    gsums = tuple(jnp.zeros((8, H), F32) for _ in range(2 * NB))
    gsums = lax.fori_loop(0, E // 32, ghost_rows, gsums, unroll=UNROLL)

    stacked = jnp.concatenate(
        [jnp.concatenate(sums[0::2], axis=0), jnp.concatenate(sums[1::2], axis=0),
         jnp.concatenate(gsums, axis=0)], axis=1)
    u0 = wide_dot(jnp.transpose(stacked), p0r_w[...])
    sig0 = 1.0 / (1.0 + jnp.exp(-u0))
    slope0[...] = sig0 * (1.0 + u0 * (1.0 - sig0))
    lent = wide_dot(h0_v[...] + u0 * sig0, wm_w[...])

    lt = jnp.transpose(lent)
    message = None
    for k in range(0, NB, 2):
        parts = [split(lt * jnp.concatenate([w1bc[m]] * 3, axis=1)) for m in (k, k + 1)]
        hi, lo = [jnp.concatenate([part[j] for part in parts], axis=1) for j in range(2)]
        a_hi, a_lo = [
            jnp.concatenate([v[:, pl.ds(m * A, A)] for m in (k, k + 1)], axis=0) for v in (ah_v, al_v)]
        both = fast_dot(jnp.concatenate([hi, lo], axis=0), a_hi)
        term = both[:CH] + both[CH:] + fast_dot(hi, a_lo)
        message = term if message is None else message + term
    hi, lo = split(message)
    wut = wut_cat[...]
    u1 = fast_dot(wut, jnp.concatenate([hi, hi], axis=0)) + fast_dot(wut[:, :CH], lo)
    sig1 = 1.0 / (1.0 + jnp.exp(-u1))
    wo2 = jnp.concatenate([wocol[...], wocol[...]], axis=1)
    hi, lo = split(wo2 * (sig1 * (1.0 + u1 * (1.0 - sig1))))
    wu = wu_cat[...]
    gm1t = fast_dot(wu, jnp.concatenate([hi, hi], axis=0)) + fast_dot(wu[:, :CH], lo)
    gm1 = jnp.transpose(gm1t)
    for k in range(NB):
        hi, lo = split(gm1 * w1[k : k + 1, :])
        gs_v[pl.ds(k * A, A), pl.ds(0, CH)] = hi
        gs_v[pl.ds(k * A, A), pl.ds(CH, CH)] = lo
    both = fast_dot(ah_v[...], gs_v[...])
    both = both + fast_dot(al_v[...], gs_v[...])
    dl = both[:, :CH] + both[:, CH:]
    l_hi, l_lo = split(lent)
    lcat = jnp.concatenate([l_hi, l_lo], axis=1)

    def radial_grad(ks, rows):
        for k in ks:
            w = w1bc[k]
            hi, lo = split(gm1t * jnp.concatenate([w, w], axis=1))
            first_row, last_row = rows
            da = fast_dot(lcat[first_row:last_row], jnp.concatenate([hi, hi], axis=0))
            da = da + fast_dot(l_hi[first_row:last_row], lo)
            at = pl.ds(first_row, last_row - first_row)
            term = da * z_v[pl.ds(k * E + first_row, last_row - first_row), :]
            q_v[at, :] = term if k == 0 else q_v[at, :] + term

    ghosts = (A, E)
    radial_grad((0, 1, 2), ghosts)
    gh1 = wide_dot(dl, wmt_w[...])
    radial_grad((3, 4, 5), ghosts)
    gh1 = jnp.concatenate([gh1[:A] + wo_v[...], gh1[A:]], axis=0)
    hi, lo = split(gh1 * slope0[...])
    p0c = p0_cat[...]
    db = fast_dot_nt(p0c, jnp.concatenate([hi, hi], axis=1)) + fast_dot_nt(p0c[:, :CH], lo)
    radial_grad((6, 7), ghosts)
    dbs[...] = jnp.concatenate([db[0:NB], db[0:NB] + db[NB : 2 * NB]], axis=0)

    factor = -2.0 / (0.2 * ROOT)

    def force_rows(start):
        rows = 16

        def step(i, carry):
            base = pl.multiple_of(start + i * rows, rows)
            at = pl.ds(base, rows)
            kind = gb[3, at, :] > 0.5
            new = list(carry)
            folds = [None] * 3
            for half in range(2):
                lanes = pl.ds(half * H, H)
                q = q_v[at, lanes]
                for k in range(NB):
                    coef = jnp.where(kind, dbs[NB + k : NB + k + 1, lanes], dbs[k : k + 1, lanes])
                    q = q + coef * z_v[pl.ds(k * E + base, rows), lanes]
                g = q * rinv_v[at, lanes] * factor
                for c in range(3):
                    f = g * (gb[c, at, :] - cen[c : c + 1, lanes])
                    folds[c] = f if half == 0 else folds[c] + f
                    new[2 * c + half] = new[2 * c + half] + folded(f)
            for c in range(3):
                fold_v[c, at, :] = folds[c]
            return tuple(new)

        return step

    def ghost_force(i, carry):
        rows = 32
        base = pl.multiple_of(i * rows, rows)
        kind = ggb[3, pl.ds(base, rows), :] > 0.5
        q = None
        for k in range(NB):
            coef = jnp.where(kind, dbs[NB + k : NB + k + 1, A:], dbs[k : k + 1, A:])
            term = coef * zg_v[pl.ds(k * E + base, rows), :]
            q = term if q is None else q + term
        g = q * rinvg_v[pl.ds(base, rows), :] * factor
        new = []
        for c in range(3):
            f = g * (ggb[c, pl.ds(base, rows), :] - ceng[c : c + 1, :])
            foldg_v[c, pl.ds(base, rows), :] = f
            new.append(carry[c] + folded(f))
        return tuple(new)

    def row_sums(start):
        return jnp.concatenate(
            [jnp.sum(jnp.transpose(fold_v[c, pl.ds(start, H), :]), axis=0, keepdims=True)
             for c in range(3)], axis=0)

    def ghost_sums(start):
        turned = [jnp.transpose(foldg_v[c, pl.ds(start, H), :]) for c in range(3)]
        return [
            jnp.concatenate([jnp.sum(t[G * part : G * part + G], axis=0, keepdims=True) for t in turned], axis=0)
            for part in range(2)
        ]

    gpulls = tuple(jnp.zeros((8, H), F32) for _ in range(3))
    gpulls = lax.fori_loop(0, E // 32, ghost_force, gpulls, unroll=UNROLL)
    pulls = tuple(jnp.zeros((8, H), F32) for _ in range(6))
    pulls = lax.fori_loop(0, 2 * G // 16, force_rows(A), pulls, unroll=UNROLL)
    lent_pull = row_sums(A) - jnp.concatenate([jnp.sum(v, axis=0, keepdims=True) for v in gpulls], axis=0)
    r_low, l_low = ghost_sums(0)
    r_high, l_high = ghost_sums(H)
    r_end, l_end = ghost_sums(2 * H)
    tx_r[...] = jnp.concatenate([r_low + jnp.where(low, lent_pull, 0.0), r_high], axis=0)
    tx_l[...] = jnp.concatenate([l_low, l_high + jnp.where(low, 0.0, lent_pull)], axis=0)
    tx_rr[...] = r_end
    tx_ll[...] = l_end
    fifth = [
        side_copy(src, dst, s5.at[i], r5.at[i], side)
        for i, (src, dst, side) in enumerate((
            (tx_r, rx_l, right), (tx_l, rx_r, left), (tx_rr, rx_ll, right2), (tx_ll, rx_rr, left2)))
    ]
    for copy in fifth:
        copy.start()
    radial_grad(range(NB), (0, A))
    pulls = lax.fori_loop(0, A // 16, force_rows(0), pulls, unroll=UNROLL)
    centre = [jnp.sum(v, axis=0, keepdims=True) for v in pulls]
    lower = jnp.concatenate(centre[0::2], axis=0) - row_sums(0) - jnp.where(low, l_end, 0.0)
    upper = jnp.concatenate(centre[1::2], axis=0) - row_sums(H) - jnp.where(low, 0.0, r_end)
    for copy in fifth:
        copy.wait_recv()
    lower = lower - jnp.where(low, rx_ll[...], 0.0)
    upper = upper - jnp.where(low, 0.0, rx_rr[...])
    pull = jnp.concatenate([lower, upper], axis=0) - (rx_l[...] + rx_r[...])
    tx6[...] = pull
    last = {lag: bead_copy(tx6, rx6.at[lag], s6.at[lag], r6.at[lag], lag) for lag in lags}
    for lag in lags:
        last[lag].start()
    ratio = beads / reduced
    totals = [ratio * table_value(-j, beads, reduced) * pull for j in range(own)]
    for lag in reversed(lags):
        last[lag].wait_recv()
        arrived = rx6[lag]
        for j in range(own):
            totals[j] = totals[j] + ratio * table_value(-own * lag - j, beads, reduced) * arrived
    for c in range(3):
        for half in range(2):
            row = 3 * half + c
            out_ref[c, :, half * H : half * H + H] = jnp.concatenate(
                [totals[j][row : row + 1] for j in range(own)], axis=0)
    for copy in list(first.values()) + aux + second + fifth + list(last.values()):
        copy.wait_send()


def solution(mesh):
    nb, ns = mesh.shape["bead"], mesh.shape["space"]

    def on_device(positions, species, neighbors, counts, send_rows, embed, w_radial, w_msg, w_upd, w_out):
        own = positions.shape[0]
        dma = pltpu.SemaphoreType.DMA

        def f32(*dims):
            return pltpu.VMEM(dims, F32)

        def i32(*dims):
            return pltpu.VMEM(dims, jnp.int32)

        def b16(*dims):
            return pltpu.VMEM(dims, BF16)

        scratch = [
            f32(3, own, A), i32(2, H), i32(K, A), i32(2, H), i32(1, H), f32(2, CH), f32(2, NB, CH),
            f32(2, CH, CH), f32(2, CH, CH), f32(1, CH),
            f32(nb, 6, H), f32(nb, 6, H),
            i32(2, H), i32(1, H), i32(2, H), i32(K, H), i32(2, H), i32(1, H), i32(2, H), i32(K, H),
            i32(2, H), i32(1, H), i32(2, H), i32(1, H),
            f32(6, H), f32(6, H), f32(6, H), f32(6, H), f32(6, H),
            i32(K, A), i32(K, H), f32(E, A), f32(E, H), f32(4, E, H), f32(4, E, H), f32(8, A), f32(8, H),
            f32(NB, CH, H), f32(CH, CH),
            b16(2 * CH, 2 * CH), b16(2 * NB, 2 * CH), b16(2 * CH, 2 * CH), b16(2 * CH, 2 * CH),
            b16(CH, 2 * CH), b16(CH, 2 * CH),
            f32(E, CH), f32(E, CH), b16(E, NB * A), b16(E, NB * A), f32(NB * E, A), f32(NB * E, H),
            f32(E, A), f32(E, H), b16(NB * A, 2 * CH), f32(E, A),
            b16(CH, 4 * H), f32(2 * NB, E), f32(3, E, H), f32(3, E, H),
            f32(6, H), f32(6, H), f32(3, H), f32(3, H), f32(6, H), f32(6, H), f32(3, H), f32(3, H),
            f32(6, H), f32(nb, 6, H),
            dma((10,)), dma((nb,)), dma((nb,)), dma((12,)), dma((12,)), dma((4,)), dma((4,)), dma((4,)), dma((4,)),
            dma((nb,)), dma((nb,)),
        ]
        forces = pl.pallas_call(
            functools.partial(kernel, nb, ns, own),
            out_shape=jax.ShapeDtypeStruct((3, own, A), F32),
            in_specs=[pl.BlockSpec(memory_space=pltpu.HBM)] * 10,
            out_specs=pl.BlockSpec(memory_space=pltpu.VMEM),
            scratch_shapes=scratch,
            compiler_params=pltpu.CompilerParams(
                collective_id=0, has_side_effects=True, vmem_limit_bytes=40 * 1024 * 1024),
        )(
            *[pltpu.with_memory_space_constraint(v, pltpu.HBM) for v in (positions.transpose(1, 0, 2), species.reshape(2, H), neighbors, counts.reshape(2, H),
            send_rows.reshape(1, H), embed, w_radial, w_msg, w_upd, w_out.reshape(1, CH))],
        )
        return forces.transpose(1, 0, 2)

    return jax.shard_map(
        on_device,
        mesh=mesh,
        in_specs=(
            P("bead", None, "space"), P("space"), P(None, "space"), P("space"), P("space"),
            P(), P(), P(), P(), P(),
        ),
        out_specs=P("bead", None, "space"),
        check_vma=False,
    )
```

```python
import functools
import math

import jax
import jax.numpy as jnp
from jax import lax
from jax.experimental import pallas as pl
from jax.experimental.pallas import tpu as pltpu
from jax.sharding import PartitionSpec as P

MESH = pl.DeviceIdType.MESH
HI = lax.Precision.HIGHEST
F32 = jnp.float32
BF16 = jnp.bfloat16

NB = 8
CH = 128
A = 256
G = 64
E = A + 2 * G
K = 32
H = 128
ROOT = math.sqrt(math.log2(math.e))
STEP = ROOT / 0.2
CENTERS = tuple(STEP * 1.5 * b / (NB - 1) for b in range(NB))
FLOOR = 0.01
UNROLL = 2


def by_distance(nb):
    def far(lag):
        dz, dx = lag % 4, lag // 4
        return -(2 * min(dz, 4 - dz) + min(dx, 4 - dx))

    return sorted(range(1, nb), key=far)


def table_value(lag, beads, reduced):
    t = lag / beads
    total = 1.0 + math.cos(math.pi * reduced * t)
    for m in range(1, reduced // 2):
        total += 2.0 * math.cos(2.0 * math.pi * m * t)
    return total / beads


def split(v):
    hi = v.astype(BF16)
    lo = (v - hi.astype(F32)).astype(BF16)
    return hi, lo


def exact_dot(a, b):
    return jnp.dot(a, b, precision=HI, preferred_element_type=F32)


def fast_dot(a, b):
    return jnp.dot(a, b, preferred_element_type=F32)


def wide(w):
    hi, lo = split(w)
    row = jnp.concatenate([hi, lo], axis=1)
    return jnp.concatenate([row, row], axis=0)


def wide_dot(a, w):
    hi, lo = split(a)
    both = fast_dot(jnp.concatenate([hi, lo], axis=1), w)
    return both[:, :CH] + both[:, CH:]


def beside(w):
    hi, lo = split(w)
    return jnp.concatenate([hi, lo], axis=1)


def left_dot(w, a):
    hi, lo = split(a)
    return fast_dot(w, jnp.concatenate([hi, hi], axis=0)) + fast_dot(w[:, :CH], lo)


def fast_dot_nt(a, b):
    return lax.dot_general(a, b, (((1,), (1,)), ((), ())), preferred_element_type=F32)


def kernel(
    nb, ns, own,
    pos_h, spc_h, nbr_h, cnt_h, snd_h, emb_h, wr_h, wm_h, wu_h, wo_h,
    out_ref,
    pos_v, spc_v, nbr_v, cnt_v, snd_v, emb_v, wr_v, wm_v, wu_v, wo_v,
    tx1, rx1,
    spc_r, snd_r, cnt_r, nbr_r, spc_l, snd_l, cnt_l, nbr_l, spc_rr, snd_rr, spc_ll, snd_ll,
    red_v, red_r, red_l, red_rr, red_ll,
    idx_v, idx_g, cnt_mat, cnt_gh, gb, ggb, cen, ceng, w1bc, wocol,
    p0rt_cat, p0_cat, wmt_cat, wmt_w, wu_cat, wut_cat,
    h0_v, slope0, ah_v, al_v, z_v, zg_v, rinv_v, rinvg_v, gs_v, q_v,
    pick_v, dbs, fold_v, foldg_v, tx_r, tx_l, tx_rr, tx_ll, rx_r, rx_l, rx_rr, rx_ll, tx6, rx6,
    load_sem, s1, r1, sa, ra, s2, r2, s5, r5, s6, r6,
):
    beads, reduced = nb * own, nb
    scale = K ** -0.5
    b = lax.axis_index("bead")
    d = lax.axis_index("space")
    left = lax.rem(d + (ns - 1), ns)
    right = lax.rem(d + 1, ns)
    left2 = lax.rem(d + (ns - 2), ns)
    right2 = lax.rem(d + 2, ns)
    peers = [lax.rem(b + lag, nb) for lag in range(nb)]
    lags = by_distance(nb)

    def bead_copy(src, dst, ss, rs, lag):
        return pltpu.make_async_remote_copy(
            src_ref=src, dst_ref=dst, send_sem=ss, recv_sem=rs,
            device_id=peers[lag] * ns + d, device_id_type=pl.DeviceIdType.LOGICAL)

    def side_copy(src, dst, ss, rs, side):
        return pltpu.make_async_remote_copy(
            src_ref=src, dst_ref=dst, send_sem=ss, recv_sem=rs,
            device_id=b * ns + side, device_id_type=pl.DeviceIdType.LOGICAL)

    barrier = pltpu.get_barrier_semaphore()
    for lag in lags:
        pl.semaphore_signal(barrier, inc=1, device_id=peers[lag] * ns + d, device_id_type=pl.DeviceIdType.LOGICAL)
    for side in (left, right, left2, right2):
        pl.semaphore_signal(barrier, inc=1, device_id=b * ns + side, device_id_type=pl.DeviceIdType.LOGICAL)

    loads = []
    for i, (src, dst) in enumerate((
        (pos_h, pos_v), (spc_h, spc_v), (snd_h, snd_v), (nbr_h, nbr_v), (cnt_h, cnt_v),
        (emb_h, emb_v), (wr_h, wr_v), (wm_h, wm_v), (wu_h, wu_v), (wo_h, wo_v),
    )):
        copy = pltpu.make_async_copy(src, dst, load_sem.at[i])
        copy.start()
        loads.append(copy)

    loads[0].wait()
    packed = []
    for j in range(own):
        packed.append(jnp.concatenate(
            [pos_v[c, j : j + 1, half * H : half * H + H] for half in range(2) for c in range(3)], axis=0))
    for lag in range(nb):
        total = None
        for j in range(own):
            term = table_value(own * lag - j, beads, reduced) * packed[j]
            total = term if total is None else total + term
        tx1[lag] = total
    for copy in loads[1:5]:
        copy.wait()
    pl.semaphore_wait(barrier, nb + 3)

    first = {lag: bead_copy(tx1.at[lag], rx1.at[lag], s1.at[lag], r1.at[lag], lag) for lag in lags}
    for lag in lags:
        first[lag].start()
    near = pl.ds(0, H)
    far = pl.ds(H, H)
    aux = [
        side_copy(src, dst, sa.at[i], ra.at[i], side)
        for i, (src, dst, side) in enumerate((
            (nbr_v.at[:, near], nbr_r, left), (nbr_v.at[:, far], nbr_l, right),
            (cnt_v, cnt_r, left), (cnt_v, cnt_l, right),
            (spc_v, spc_r, left), (spc_v, spc_l, right), (spc_v, spc_rr, left2), (spc_v, spc_ll, right2),
            (snd_v, snd_r, left), (snd_v, snd_l, right), (snd_v, snd_rr, left2), (snd_v, snd_ll, right2),
        ))
    ]
    for copy in aux:
        copy.start()

    def rows_named(n, count):
        n = jnp.where(n >= A + G, n - G, jnp.where(n >= A, n + G, n))
        slot = lax.broadcasted_iota(jnp.int32, n.shape, 0)
        return jnp.where(slot < count, n, -1)

    def count_rows(idx, mat, width, rows):
        def step(i, carry):
            base = pl.multiple_of(i * rows, rows)
            row = lax.broadcasted_iota(jnp.int32, (rows, width), 0) + base
            acc = jnp.zeros((rows, width), F32)
            for k in range(K):
                acc = acc + jnp.where(idx[k : k + 1, :] == row, 1.0, 0.0)
            mat[pl.ds(base, rows), :] = acc
            return carry

        lax.fori_loop(0, E // rows, step, 0)

    idx_v[...] = rows_named(nbr_v[...], jnp.concatenate([cnt_v[0:1, :], cnt_v[1:2, :]], axis=1))
    count_rows(idx_v, cnt_mat, A, 32)

    for copy in loads[5:]:
        copy.wait()
    zeros6 = jnp.zeros((6, CH), F32)
    emb8 = jnp.concatenate([emb_v[...], zeros6], axis=0)
    table = exact_dot(emb8, wm_v[0])
    w0 = wr_v[0] * scale
    rows0 = jnp.concatenate([w0 * table[0:1], w0 * (table[1:2] - table[0:1])], axis=0)
    p0 = exact_dot(rows0, wu_v[0])
    p0_hi, p0_lo = split(p0)
    p0_cat[...] = jnp.concatenate([p0_hi, p0_lo], axis=1)
    p0rt_cat[...] = beside(jnp.transpose(jnp.concatenate(
        [jnp.broadcast_to(p0[j : j + 1, :], (8, CH)) for j in range(2 * NB)], axis=0)))
    w1 = wr_v[1] * scale
    w1t = jnp.transpose(jnp.concatenate([w1, jnp.zeros((CH - NB, CH), F32)], axis=0))
    for k in range(NB):
        w1bc[k] = jnp.broadcast_to(w1t[:, k : k + 1], (CH, H))
    wm_turned = jnp.transpose(wm_v[1])
    wmt_cat[...] = beside(wm_turned)
    wmt_w[...] = wide(wm_turned)
    wu_cat[...] = beside(wu_v[1])
    wut_cat[...] = beside(jnp.transpose(wu_v[1]))
    wocol[...] = jnp.transpose(jnp.broadcast_to(wo_v[...], (CH, CH)))

    lane = lax.broadcasted_iota(jnp.int32, (1, H), 1)
    low = lane < G

    row = lax.broadcasted_iota(jnp.int32, (CH, 4 * H), 0)
    spot = lax.broadcasted_iota(jnp.int32, (CH, 4 * H), 1)
    value = spot // H + jnp.where(spot % H < G, 0, 4)
    pick_v[...] = jnp.where((row < 24) & (row % 8 == value), 1.0, 0.0).astype(BF16)

    red = tx1[0]
    for lag in lags:
        first[lag].wait_recv()
        red = red + rx1[lag]
    red_v[...] = red
    second = [
        side_copy(red_v, dst, s2.at[i], r2.at[i], side)
        for i, (dst, side) in enumerate(((red_r, left), (red_l, right), (red_rr, left2), (red_ll, right2)))
    ]
    for copy in second:
        copy.start()

    for copy in aux:
        copy.wait_recv()
    idx_g[...] = rows_named(
        jnp.where(low, nbr_r[...], nbr_l[...]), jnp.where(low, cnt_r[0:1, :], cnt_l[1:2, :]))
    count_rows(idx_g, cnt_gh, H, 64)
    natural = lax.broadcasted_iota(jnp.int32, (H, H), 0)

    def reorder(from_right, from_left, rows):
        order = jnp.where(low, from_right, from_left - (A - H))
        return fast_dot(jnp.where(natural == order, 1.0, 0.0).astype(BF16), rows)

    cnt_mat[pl.ds(A, 2 * G), :] = reorder(snd_r[...], snd_l[...], cnt_mat[pl.ds(A, 2 * G), :].astype(BF16))
    rows_gh = cnt_gh[pl.ds(A, 2 * G), :].astype(BF16)
    cnt_gh[pl.ds(A, 2 * G), :] = jnp.where(
        low, reorder(snd_rr[...], snd_v[...], rows_gh), reorder(snd_v[...], snd_ll[...], rows_gh))
    kind_own = spc_v[...].astype(F32)
    kind_r, kind_l = spc_r[...].astype(F32), spc_l[...].astype(F32)
    kind_gh = jnp.where(low, kind_r[0:1], kind_l[1:2])
    kind_rg = jnp.where(low, spc_rr[0:1, :].astype(F32), kind_own[1:2])
    kind_lg = jnp.where(low, kind_own[0:1], spc_ll[1:2, :].astype(F32))
    zrest = jnp.zeros((CH - 4, H), F32)
    kinds = [jnp.transpose(jnp.broadcast_to(emb_v[t : t + 1, :], (H, CH))) for t in range(2)]
    for part, kind in enumerate((kind_own[0:1], kind_own[1:2], kind_gh)):
        h0_v[:, pl.ds(part * H, H)] = jnp.where(kind > 0.5, kinds[1], kinds[0])
    cen[...] = jnp.concatenate(
        [jnp.concatenate([red[0:3], red[3:6]], axis=1), jnp.zeros((5, A), F32)], axis=0)

    def spread_rows(part, pieces):
        col = jnp.transpose(jnp.concatenate(pieces + [zrest], axis=0))
        for c in range(4):
            gb[c, pl.ds(part * H, H), :] = jnp.broadcast_to(col[:, c : c + 1], (H, H))

    for half in range(2):
        spread_rows(half, [red[3 * half : 3 * half + 3], kind_own[half : half + 1]])

    def folded(v):
        total = v[0:8]
        for r in range(8, v.shape[0], 8):
            total = total + v[r : r + 8]
        return total

    def pair_rows(start):
        rows = 16

        def step(i, carry):
            base = pl.multiple_of(start + i * rows, rows)
            at = pl.ds(base, rows)
            gx, gy, gz, kind = [gb[c, at, :] for c in range(4)]
            sums = list(carry)
            for half in range(2):
                lanes = pl.ds(half * H, H)
                dx, dy, dz = gx - cen[0:1, lanes], gy - cen[1:2, lanes], gz - cen[2:3, lanes]
                square = dx * dx + dy * dy + dz * dz + FLOOR
                rinv = lax.rsqrt(square)
                x = square * rinv * STEP
                rinv_v[at, lanes] = rinv
                c = cnt_mat[at, lanes]
                for k in range(NB):
                    off = x - CENTERS[k]
                    a = c * jnp.exp2(-(off * off))
                    hi, lo = split(a)
                    spot = pl.ds(k * A + half * H, H)
                    ah_v[at, spot] = hi
                    al_v[at, spot] = lo
                    z_v[pl.ds(k * E + base, rows), lanes] = a * off
                    sums[2 * k + half] = sums[2 * k + half] + folded(a)
                    j = 2 * NB + 2 * k + half
                    sums[j] = sums[j] + folded(a * kind)
            return tuple(sums)

        return step

    sums = tuple(jnp.zeros((8, H), F32) for _ in range(4 * NB))
    sums = lax.fori_loop(0, A // 16, pair_rows(0), sums, unroll=UNROLL)
    for copy in second:
        copy.wait_recv()

    def shifted(at_left, at_right, values):
        shift = jnp.where(low, jnp.where(at_right, float(ns), 0.0), jnp.where(at_left, -float(ns), 0.0))
        first_row = lax.broadcasted_iota(jnp.int32, (3, H), 0) == 0
        return values + jnp.where(first_row, shift, 0.0)

    borrowed = jnp.where(low, red_r[0:3, :], red_l[3:6, :])
    ceng[...] = jnp.concatenate([borrowed, jnp.zeros((5, H), F32)], axis=0)
    ghost = shifted(d == 0, d == ns - 1, borrowed)
    ghost_r = shifted(right == 0, right == ns - 1, jnp.where(low, red_rr[0:3, :], red[3:6]))
    ghost_l = shifted(left == 0, left == ns - 1, jnp.where(low, red[0:3], red_ll[3:6, :]))
    spread_rows(2, [ghost, kind_gh])
    for part, pieces in enumerate((
        (red_r[0:3, :], kind_r[0:1], red_l[0:3, :], kind_l[0:1]),
        (red_r[3:6, :], kind_r[1:2], red_l[3:6, :], kind_l[1:2]),
        (ghost_r, kind_rg, ghost_l, kind_lg),
    )):
        rest = jnp.concatenate(list(pieces), axis=0)
        layers = []
        for _ in range(3):
            layer = rest.astype(BF16).astype(F32)
            layers.append(layer)
            rest = rest - layer
        col = jnp.transpose(jnp.concatenate(layers + [jnp.zeros((CH - 24, H), F32)], axis=0)).astype(BF16)
        spread = fast_dot(col, pick_v[...])
        for c in range(4):
            ggb[c, pl.ds(part * H, H), :] = spread[:, c * H : c * H + H]

    def ghost_rows(i, carry):
        rows = 32
        base = pl.multiple_of(i * rows, rows)
        dx, dy, dz = [ggb[c, pl.ds(base, rows), :] - ceng[c : c + 1, :] for c in range(3)]
        kind = ggb[3, pl.ds(base, rows), :]
        square = dx * dx + dy * dy + dz * dz + FLOOR
        rinv = lax.rsqrt(square)
        x = square * rinv * STEP
        rinvg_v[pl.ds(base, rows), :] = rinv
        c = cnt_gh[pl.ds(base, rows), :]
        sums = list(carry)
        for k in range(NB):
            off = x - CENTERS[k]
            a = c * jnp.exp2(-(off * off))
            zg_v[pl.ds(k * E + base, rows), :] = a * off
            s = a * kind
            sums[k] = sums[k] + folded(a)
            sums[NB + k] = sums[NB + k] + folded(s)
        return tuple(sums)

    sums = lax.fori_loop(0, 2 * G // 16, pair_rows(A), sums, unroll=UNROLL)
    gsums = tuple(jnp.zeros((8, H), F32) for _ in range(2 * NB))
    gsums = lax.fori_loop(0, E // 32, ghost_rows, gsums, unroll=UNROLL)

    stacked = jnp.concatenate(
        [jnp.concatenate(sums[0::2], axis=0), jnp.concatenate(sums[1::2], axis=0),
         jnp.concatenate(gsums, axis=0)], axis=1)
    u0 = left_dot(p0rt_cat[...], stacked)
    sig0 = 1.0 / (1.0 + jnp.exp(-u0))
    lt = left_dot(wmt_cat[...], h0_v[...] + u0 * sig0)

    message = None
    for k in range(0, NB, 2):
        parts = [split(lt * jnp.concatenate([w1bc[m]] * 3, axis=1)) for m in (k, k + 1)]
        hi, lo = [jnp.concatenate([part[j] for part in parts], axis=1) for j in range(2)]
        a_hi, a_lo = [
            jnp.concatenate([v[:, pl.ds(m * A, A)] for m in (k, k + 1)], axis=0) for v in (ah_v, al_v)]
        both = fast_dot(jnp.concatenate([hi, lo], axis=0), a_hi)
        term = both[:CH] + both[CH:] + fast_dot(hi, a_lo)
        message = term if message is None else message + term
    slope0[...] = jnp.transpose(sig0 * (1.0 + u0 * (1.0 - sig0)))
    lent = jnp.transpose(lt)
    l_hi, l_lo = split(lent)
    lcat = jnp.concatenate([l_hi, l_lo], axis=1)
    u1 = left_dot(wut_cat[...], message)
    sig1 = 1.0 / (1.0 + jnp.exp(-u1))
    wo2 = jnp.concatenate([wocol[...], wocol[...]], axis=1)
    gm1t = left_dot(wu_cat[...], wo2 * (sig1 * (1.0 + u1 * (1.0 - sig1))))
    gm1 = jnp.transpose(gm1t)
    for k in range(NB):
        hi, lo = split(gm1 * w1[k : k + 1, :])
        gs_v[pl.ds(k * A, A), pl.ds(0, CH)] = hi
        gs_v[pl.ds(k * A, A), pl.ds(CH, CH)] = lo
    both = fast_dot(ah_v[...], gs_v[...])
    both = both + fast_dot(al_v[...], gs_v[...])
    dl = both[:, :CH] + both[:, CH:]

    def radial_grad(ks, rows):
        for k in ks:
            w = w1bc[k]
            hi, lo = split(gm1t * jnp.concatenate([w, w], axis=1))
            first_row, last_row = rows
            da = fast_dot(lcat[first_row:last_row], jnp.concatenate([hi, hi], axis=0))
            da = da + fast_dot(l_hi[first_row:last_row], lo)
            at = pl.ds(first_row, last_row - first_row)
            term = da * z_v[pl.ds(k * E + first_row, last_row - first_row), :]
            q_v[at, :] = term if k == 0 else q_v[at, :] + term

    ghosts = (A, E)
    radial_grad((0, 1, 2), ghosts)
    gh1 = wide_dot(dl, wmt_w[...])
    radial_grad((3, 4, 5), ghosts)
    gh1 = jnp.concatenate([gh1[:A] + wo_v[...], gh1[A:]], axis=0)
    hi, lo = split(gh1 * slope0[...])
    p0c = p0_cat[...]
    db = fast_dot_nt(p0c, jnp.concatenate([hi, hi], axis=1)) + fast_dot_nt(p0c[:, :CH], lo)
    radial_grad((6, 7), ghosts)
    dbs[...] = jnp.concatenate([db[0:NB], db[0:NB] + db[NB : 2 * NB]], axis=0)

    factor = -2.0 / (0.2 * ROOT)

    def force_rows(start):
        rows = 16

        def step(i, carry):
            base = pl.multiple_of(start + i * rows, rows)
            at = pl.ds(base, rows)
            kind = gb[3, at, :] > 0.5
            new = list(carry)
            folds = [None] * 3
            for half in range(2):
                lanes = pl.ds(half * H, H)
                q = q_v[at, lanes]
                for k in range(NB):
                    coef = jnp.where(kind, dbs[NB + k : NB + k + 1, lanes], dbs[k : k + 1, lanes])
                    q = q + coef * z_v[pl.ds(k * E + base, rows), lanes]
                g = q * rinv_v[at, lanes] * factor
                for c in range(3):
                    f = g * (gb[c, at, :] - cen[c : c + 1, lanes])
                    folds[c] = f if half == 0 else folds[c] + f
                    new[2 * c + half] = new[2 * c + half] + folded(f)
            for c in range(3):
                fold_v[c, at, :] = folds[c]
            return tuple(new)

        return step

    def ghost_force(i, carry):
        rows = 32
        base = pl.multiple_of(i * rows, rows)
        kind = ggb[3, pl.ds(base, rows), :] > 0.5
        q = None
        for k in range(NB):
            coef = jnp.where(kind, dbs[NB + k : NB + k + 1, A:], dbs[k : k + 1, A:])
            term = coef * zg_v[pl.ds(k * E + base, rows), :]
            q = term if q is None else q + term
        g = q * rinvg_v[pl.ds(base, rows), :] * factor
        new = []
        for c in range(3):
            f = g * (ggb[c, pl.ds(base, rows), :] - ceng[c : c + 1, :])
            foldg_v[c, pl.ds(base, rows), :] = f
            new.append(carry[c] + folded(f))
        return tuple(new)

    def row_sums(start):
        return jnp.concatenate(
            [jnp.sum(jnp.transpose(fold_v[c, pl.ds(start, H), :]), axis=0, keepdims=True)
             for c in range(3)], axis=0)

    def ghost_sums(start):
        turned = [jnp.transpose(foldg_v[c, pl.ds(start, H), :]) for c in range(3)]
        return [
            jnp.concatenate([jnp.sum(t[G * part : G * part + G], axis=0, keepdims=True) for t in turned], axis=0)
            for part in range(2)
        ]

    gpulls = tuple(jnp.zeros((8, H), F32) for _ in range(3))
    gpulls = lax.fori_loop(0, E // 32, ghost_force, gpulls, unroll=UNROLL)
    pulls = tuple(jnp.zeros((8, H), F32) for _ in range(6))
    pulls = lax.fori_loop(0, 2 * G // 16, force_rows(A), pulls, unroll=UNROLL)
    lent_pull = row_sums(A) - jnp.concatenate([jnp.sum(v, axis=0, keepdims=True) for v in gpulls], axis=0)
    r_low, l_low = ghost_sums(0)
    r_high, l_high = ghost_sums(H)
    r_end, l_end = ghost_sums(2 * H)
    tx_r[...] = jnp.concatenate([r_low + jnp.where(low, lent_pull, 0.0), r_high], axis=0)
    tx_l[...] = jnp.concatenate([l_low, l_high + jnp.where(low, 0.0, lent_pull)], axis=0)
    tx_rr[...] = r_end
    tx_ll[...] = l_end
    fifth = [
        side_copy(src, dst, s5.at[i], r5.at[i], side)
        for i, (src, dst, side) in enumerate((
            (tx_r, rx_l, right), (tx_l, rx_r, left), (tx_rr, rx_ll, right2), (tx_ll, rx_rr, left2)))
    ]
    for copy in fifth:
        copy.start()
    radial_grad(range(NB), (0, A))
    pulls = lax.fori_loop(0, A // 16, force_rows(0), pulls, unroll=UNROLL)
    centre = [jnp.sum(v, axis=0, keepdims=True) for v in pulls]
    lower = jnp.concatenate(centre[0::2], axis=0) - row_sums(0) - jnp.where(low, l_end, 0.0)
    upper = jnp.concatenate(centre[1::2], axis=0) - row_sums(H) - jnp.where(low, 0.0, r_end)
    for copy in fifth:
        copy.wait_recv()
    lower = lower - jnp.where(low, rx_ll[...], 0.0)
    upper = upper - jnp.where(low, 0.0, rx_rr[...])
    pull = jnp.concatenate([lower, upper], axis=0) - (rx_l[...] + rx_r[...])
    tx6[...] = pull
    last = {lag: bead_copy(tx6, rx6.at[lag], s6.at[lag], r6.at[lag], lag) for lag in lags}
    for lag in lags:
        last[lag].start()
    ratio = beads / reduced
    totals = [ratio * table_value(-j, beads, reduced) * pull for j in range(own)]
    for lag in reversed(lags):
        last[lag].wait_recv()
        arrived = rx6[lag]
        for j in range(own):
            totals[j] = totals[j] + ratio * table_value(-own * lag - j, beads, reduced) * arrived
    for c in range(3):
        for half in range(2):
            row = 3 * half + c
            out_ref[c, :, half * H : half * H + H] = jnp.concatenate(
                [totals[j][row : row + 1] for j in range(own)], axis=0)
    for copy in list(first.values()) + aux + second + fifth + list(last.values()):
        copy.wait_send()


def solution(mesh):
    nb, ns = mesh.shape["bead"], mesh.shape["space"]

    def on_device(positions, species, neighbors, counts, send_rows, embed, w_radial, w_msg, w_upd, w_out):
        own = positions.shape[0]
        dma = pltpu.SemaphoreType.DMA

        def f32(*dims):
            return pltpu.VMEM(dims, F32)

        def i32(*dims):
            return pltpu.VMEM(dims, jnp.int32)

        def b16(*dims):
            return pltpu.VMEM(dims, BF16)

        scratch = [
            f32(3, own, A), i32(2, H), i32(K, A), i32(2, H), i32(1, H), f32(2, CH), f32(2, NB, CH),
            f32(2, CH, CH), f32(2, CH, CH), f32(1, CH),
            f32(nb, 6, H), f32(nb, 6, H),
            i32(2, H), i32(1, H), i32(2, H), i32(K, H), i32(2, H), i32(1, H), i32(2, H), i32(K, H),
            i32(2, H), i32(1, H), i32(2, H), i32(1, H),
            f32(6, H), f32(6, H), f32(6, H), f32(6, H), f32(6, H),
            i32(K, A), i32(K, H), f32(E, A), f32(E, H), f32(4, E, H), f32(4, E, H), f32(8, A), f32(8, H),
            f32(NB, CH, H), f32(CH, CH),
            b16(CH, 2 * CH), b16(2 * NB, 2 * CH), b16(CH, 2 * CH), b16(2 * CH, 2 * CH),
            b16(CH, 2 * CH), b16(CH, 2 * CH),
            f32(CH, E), f32(E, CH), b16(E, NB * A), b16(E, NB * A), f32(NB * E, A), f32(NB * E, H),
            f32(E, A), f32(E, H), b16(NB * A, 2 * CH), f32(E, A),
            b16(CH, 4 * H), f32(2 * NB, E), f32(3, E, H), f32(3, E, H),
            f32(6, H), f32(6, H), f32(3, H), f32(3, H), f32(6, H), f32(6, H), f32(3, H), f32(3, H),
            f32(6, H), f32(nb, 6, H),
            dma((10,)), dma((nb,)), dma((nb,)), dma((12,)), dma((12,)), dma((4,)), dma((4,)), dma((4,)), dma((4,)),
            dma((nb,)), dma((nb,)),
        ]
        forces = pl.pallas_call(
            functools.partial(kernel, nb, ns, own),
            out_shape=jax.ShapeDtypeStruct((3, own, A), F32),
            in_specs=[pl.BlockSpec(memory_space=pltpu.HBM)] * 10,
            out_specs=pl.BlockSpec(memory_space=pltpu.VMEM),
            scratch_shapes=scratch,
            compiler_params=pltpu.CompilerParams(
                collective_id=0, has_side_effects=True, vmem_limit_bytes=40 * 1024 * 1024),
        )(
            *[pltpu.with_memory_space_constraint(v, pltpu.HBM) for v in (positions.transpose(1, 0, 2), species.reshape(2, H), neighbors, counts.reshape(2, H),
            send_rows.reshape(1, H), embed, w_radial, w_msg, w_upd, w_out.reshape(1, CH))],
        )
        return forces.transpose(1, 0, 2)

    return jax.shard_map(
        on_device,
        mesh=mesh,
        in_specs=(
            P("bead", None, "space"), P("space"), P(None, "space"), P("space"), P("space"),
            P(), P(), P(), P(), P(),
        ),
        out_specs=P("bead", None, "space"),
        check_vma=False,
    )
```

```python
import functools
import math

import jax
import jax.numpy as jnp
from jax import lax
from jax.experimental import pallas as pl
from jax.experimental.pallas import tpu as pltpu
from jax.sharding import PartitionSpec as P

MESH = pl.DeviceIdType.MESH
HI = lax.Precision.HIGHEST
F32 = jnp.float32
BF16 = jnp.bfloat16

NB = 8
CH = 128
A = 256
G = 64
E = A + 2 * G
K = 32
H = 128
ROOT = math.sqrt(math.log2(math.e))
STEP = ROOT / 0.2
CENTERS = tuple(STEP * 1.5 * b / (NB - 1) for b in range(NB))
FLOOR = 0.01
UNROLL = 2


def by_distance(nb):
    def far(lag):
        dz, dx = lag % 4, lag // 4
        return -(2 * min(dz, 4 - dz) + min(dx, 4 - dx))

    return sorted(range(1, nb), key=far)


def table_value(lag, beads, reduced):
    t = lag / beads
    total = 1.0 + math.cos(math.pi * reduced * t)
    for m in range(1, reduced // 2):
        total += 2.0 * math.cos(2.0 * math.pi * m * t)
    return total / beads


def split(v):
    hi = v.astype(BF16)
    lo = (v - hi.astype(F32)).astype(BF16)
    return hi, lo


def exact_dot(a, b):
    return jnp.dot(a, b, precision=HI, preferred_element_type=F32)


def fast_dot(a, b):
    return jnp.dot(a, b, preferred_element_type=F32)


def wide(w):
    hi, lo = split(w)
    row = jnp.concatenate([hi, lo], axis=1)
    return jnp.concatenate([row, row], axis=0)


def wide_dot(a, w):
    hi, lo = split(a)
    both = fast_dot(jnp.concatenate([hi, lo], axis=1), w)
    return both[:, :CH] + both[:, CH:]


def beside(w):
    hi, lo = split(w)
    return jnp.concatenate([hi, lo], axis=1)


def left_dot(w, a):
    hi, lo = split(a)
    return fast_dot(w, jnp.concatenate([hi, hi], axis=0)) + fast_dot(w[:, :CH], lo)


def fast_dot_nt(a, b):
    return lax.dot_general(a, b, (((1,), (1,)), ((), ())), preferred_element_type=F32)


def kernel(
    nb, ns, own,
    pos_h, spc_h, nbr_h, cnt_h, snd_h, emb_h, wr_h, wm_h, wu_h, wo_h,
    out_ref,
    pos_v, spc_v, nbr_v, cnt_v, snd_v, emb_v, wr_v, wm_v, wu_v, wo_v,
    tx1, rx1,
    spc_r, snd_r, cnt_r, nbr_r, spc_l, snd_l, cnt_l, nbr_l, spc_rr, snd_rr, spc_ll, snd_ll,
    red_v, red_r, red_l, red_rr, red_ll,
    idx_v, idx_g, cnt_mat, cnt_gh, gb, ggb, cen, ceng, w1bc, wocol,
    p0rt_cat, p0_cat, wmt_cat, wmt_w, wu_cat, wut_cat,
    h0_v, slope0, ah_v, al_v, z_v, zg_v, rinv_v, rinvg_v, gs_v, q_v,
    pick_v, dbs, fold_v, foldg_v, tx_r, tx_l, tx_rr, tx_ll, rx_r, rx_l, rx_rr, rx_ll, tx6, rx6,
    load_sem, s1, r1, sa, ra, s2, r2, s5, r5, s6, r6,
):
    beads, reduced = nb * own, nb
    scale = K ** -0.5
    b = lax.axis_index("bead")
    d = lax.axis_index("space")
    left = lax.rem(d + (ns - 1), ns)
    right = lax.rem(d + 1, ns)
    left2 = lax.rem(d + (ns - 2), ns)
    right2 = lax.rem(d + 2, ns)
    peers = [lax.rem(b + lag, nb) for lag in range(nb)]
    lags = by_distance(nb)

    def bead_copy(src, dst, ss, rs, lag):
        return pltpu.make_async_remote_copy(
            src_ref=src, dst_ref=dst, send_sem=ss, recv_sem=rs,
            device_id=peers[lag] * ns + d, device_id_type=pl.DeviceIdType.LOGICAL)

    def side_copy(src, dst, ss, rs, side):
        return pltpu.make_async_remote_copy(
            src_ref=src, dst_ref=dst, send_sem=ss, recv_sem=rs,
            device_id=b * ns + side, device_id_type=pl.DeviceIdType.LOGICAL)

    barrier = pltpu.get_barrier_semaphore()
    for lag in lags:
        pl.semaphore_signal(barrier, inc=1, device_id=peers[lag] * ns + d, device_id_type=pl.DeviceIdType.LOGICAL)
    for side in (left, right, left2, right2):
        pl.semaphore_signal(barrier, inc=1, device_id=b * ns + side, device_id_type=pl.DeviceIdType.LOGICAL)

    loads = []
    for i, (src, dst) in enumerate((
        (pos_h, pos_v), (spc_h, spc_v), (snd_h, snd_v), (nbr_h, nbr_v), (cnt_h, cnt_v),
        (emb_h, emb_v), (wr_h, wr_v), (wm_h, wm_v), (wu_h, wu_v), (wo_h, wo_v),
    )):
        copy = pltpu.make_async_copy(src, dst, load_sem.at[i])
        copy.start()
        loads.append(copy)

    loads[0].wait()
    packed = []
    for j in range(own):
        packed.append(jnp.concatenate(
            [pos_v[c, j : j + 1, half * H : half * H + H] for half in range(2) for c in range(3)], axis=0))
    for lag in range(nb):
        total = None
        for j in range(own):
            term = table_value(own * lag - j, beads, reduced) * packed[j]
            total = term if total is None else total + term
        tx1[lag] = total
    for copy in loads[1:5]:
        copy.wait()
    pl.semaphore_wait(barrier, nb + 3)

    first = {lag: bead_copy(tx1.at[lag], rx1.at[lag], s1.at[lag], r1.at[lag], lag) for lag in lags}
    for lag in lags:
        first[lag].start()
    near = pl.ds(0, H)
    far = pl.ds(H, H)
    aux = [
        side_copy(src, dst, sa.at[i], ra.at[i], side)
        for i, (src, dst, side) in enumerate((
            (nbr_v.at[:, near], nbr_r, left), (nbr_v.at[:, far], nbr_l, right),
            (cnt_v, cnt_r, left), (cnt_v, cnt_l, right),
            (spc_v, spc_r, left), (spc_v, spc_l, right), (spc_v, spc_rr, left2), (spc_v, spc_ll, right2),
            (snd_v, snd_r, left), (snd_v, snd_l, right), (snd_v, snd_rr, left2), (snd_v, snd_ll, right2),
        ))
    ]
    for copy in aux:
        copy.start()

    def rows_named(n, count):
        n = jnp.where(n >= A + G, n - G, jnp.where(n >= A, n + G, n))
        slot = lax.broadcasted_iota(jnp.int32, n.shape, 0)
        return jnp.where(slot < count, n, -1)

    def count_rows(idx, mat, width, rows):
        def step(i, carry):
            base = pl.multiple_of(i * rows, rows)
            row = lax.broadcasted_iota(jnp.int32, (rows, width), 0) + base
            acc = jnp.zeros((rows, width), F32)
            for k in range(K):
                acc = acc + jnp.where(idx[k : k + 1, :] == row, 1.0, 0.0)
            mat[pl.ds(base, rows), :] = acc
            return carry

        lax.fori_loop(0, E // rows, step, 0)

    idx_v[...] = rows_named(nbr_v[...], jnp.concatenate([cnt_v[0:1, :], cnt_v[1:2, :]], axis=1))
    count_rows(idx_v, cnt_mat, A, 32)

    for copy in loads[5:]:
        copy.wait()
    zeros6 = jnp.zeros((6, CH), F32)
    emb8 = jnp.concatenate([emb_v[...], zeros6], axis=0)
    table = exact_dot(emb8, wm_v[0])
    w0 = wr_v[0] * scale
    rows0 = jnp.concatenate([w0 * table[0:1], w0 * (table[1:2] - table[0:1])], axis=0)
    p0 = exact_dot(rows0, wu_v[0])
    p0_hi, p0_lo = split(p0)
    p0_cat[...] = jnp.concatenate([p0_hi, p0_lo], axis=1)
    p0rt_cat[...] = beside(jnp.transpose(jnp.concatenate(
        [jnp.broadcast_to(p0[j : j + 1, :], (8, CH)) for j in range(2 * NB)], axis=0)))
    w1 = wr_v[1] * scale
    w1t = jnp.transpose(jnp.concatenate([w1, jnp.zeros((CH - NB, CH), F32)], axis=0))
    for k in range(NB):
        w1bc[k] = jnp.broadcast_to(w1t[:, k : k + 1], (CH, H))
    wm_turned = jnp.transpose(wm_v[1])
    wmt_cat[...] = beside(wm_turned)
    wmt_w[...] = wide(wm_turned)
    wu_cat[...] = beside(wu_v[1])
    wut_cat[...] = beside(jnp.transpose(wu_v[1]))
    wocol[...] = jnp.transpose(jnp.broadcast_to(wo_v[...], (CH, CH)))

    lane = lax.broadcasted_iota(jnp.int32, (1, H), 1)
    low = lane < G

    row = lax.broadcasted_iota(jnp.int32, (CH, 4 * H), 0)
    spot = lax.broadcasted_iota(jnp.int32, (CH, 4 * H), 1)
    value = spot // H + jnp.where(spot % H < G, 0, 4)
    pick_v[...] = jnp.where((row < 24) & (row % 8 == value), 1.0, 0.0).astype(BF16)

    red = tx1[0]
    for lag in lags:
        first[lag].wait_recv()
        red = red + rx1[lag]
    red_v[...] = red
    second = [
        side_copy(red_v, dst, s2.at[i], r2.at[i], side)
        for i, (dst, side) in enumerate(((red_rr, left2), (red_ll, right2), (red_r, left), (red_l, right)))
    ]
    for copy in second:
        copy.start()

    for copy in aux:
        copy.wait_recv()
    idx_g[...] = rows_named(
        jnp.where(low, nbr_r[...], nbr_l[...]), jnp.where(low, cnt_r[0:1, :], cnt_l[1:2, :]))
    count_rows(idx_g, cnt_gh, H, 64)
    natural = lax.broadcasted_iota(jnp.int32, (H, H), 0)

    def reorder(from_right, from_left, rows):
        order = jnp.where(low, from_right, from_left - (A - H))
        return fast_dot(jnp.where(natural == order, 1.0, 0.0).astype(BF16), rows)

    cnt_mat[pl.ds(A, 2 * G), :] = reorder(snd_r[...], snd_l[...], cnt_mat[pl.ds(A, 2 * G), :].astype(BF16))
    rows_gh = cnt_gh[pl.ds(A, 2 * G), :].astype(BF16)
    cnt_gh[pl.ds(A, 2 * G), :] = jnp.where(
        low, reorder(snd_rr[...], snd_v[...], rows_gh), reorder(snd_v[...], snd_ll[...], rows_gh))
    kind_own = spc_v[...].astype(F32)
    kind_r, kind_l = spc_r[...].astype(F32), spc_l[...].astype(F32)
    kind_gh = jnp.where(low, kind_r[0:1], kind_l[1:2])
    kind_rg = jnp.where(low, spc_rr[0:1, :].astype(F32), kind_own[1:2])
    kind_lg = jnp.where(low, kind_own[0:1], spc_ll[1:2, :].astype(F32))
    zrest = jnp.zeros((CH - 4, H), F32)
    kinds = [jnp.transpose(jnp.broadcast_to(emb_v[t : t + 1, :], (H, CH))) for t in range(2)]
    for part, kind in enumerate((kind_own[0:1], kind_own[1:2], kind_gh)):
        h0_v[:, pl.ds(part * H, H)] = jnp.where(kind > 0.5, kinds[1], kinds[0])
    cen[...] = jnp.concatenate(
        [jnp.concatenate([red[0:3], red[3:6]], axis=1), jnp.zeros((5, A), F32)], axis=0)

    def spread_rows(part, pieces):
        col = jnp.transpose(jnp.concatenate(pieces + [zrest], axis=0))
        for c in range(4):
            gb[c, pl.ds(part * H, H), :] = jnp.broadcast_to(col[:, c : c + 1], (H, H))

    for half in range(2):
        spread_rows(half, [red[3 * half : 3 * half + 3], kind_own[half : half + 1]])

    def folded(v):
        total = v[0:8]
        for r in range(8, v.shape[0], 8):
            total = total + v[r : r + 8]
        return total

    def pair_rows(start):
        rows = 16

        def step(i, carry):
            base = pl.multiple_of(start + i * rows, rows)
            at = pl.ds(base, rows)
            gx, gy, gz, kind = [gb[c, at, :] for c in range(4)]
            sums = list(carry)
            for half in range(2):
                lanes = pl.ds(half * H, H)
                dx, dy, dz = gx - cen[0:1, lanes], gy - cen[1:2, lanes], gz - cen[2:3, lanes]
                square = dx * dx + dy * dy + dz * dz + FLOOR
                rinv = lax.rsqrt(square)
                x = square * rinv * STEP
                rinv_v[at, lanes] = rinv
                c = cnt_mat[at, lanes]
                for k in range(NB):
                    off = x - CENTERS[k]
                    a = c * jnp.exp2(-(off * off))
                    hi, lo = split(a)
                    spot = pl.ds(k * A + half * H, H)
                    ah_v[at, spot] = hi
                    al_v[at, spot] = lo
                    z_v[pl.ds(k * E + base, rows), lanes] = a * off
                    sums[2 * k + half] = sums[2 * k + half] + folded(a)
                    j = 2 * NB + 2 * k + half
                    sums[j] = sums[j] + folded(a * kind)
            return tuple(sums)

        return step

    sums = tuple(jnp.zeros((8, H), F32) for _ in range(4 * NB))
    sums = lax.fori_loop(0, A // 16, pair_rows(0), sums, unroll=UNROLL)
    for copy in second:
        copy.wait_recv()

    def shifted(at_left, at_right, values):
        shift = jnp.where(low, jnp.where(at_right, float(ns), 0.0), jnp.where(at_left, -float(ns), 0.0))
        first_row = lax.broadcasted_iota(jnp.int32, (3, H), 0) == 0
        return values + jnp.where(first_row, shift, 0.0)

    borrowed = jnp.where(low, red_r[0:3, :], red_l[3:6, :])
    ceng[...] = jnp.concatenate([borrowed, jnp.zeros((5, H), F32)], axis=0)
    ghost = shifted(d == 0, d == ns - 1, borrowed)
    ghost_r = shifted(right == 0, right == ns - 1, jnp.where(low, red_rr[0:3, :], red[3:6]))
    ghost_l = shifted(left == 0, left == ns - 1, jnp.where(low, red[0:3], red_ll[3:6, :]))
    spread_rows(2, [ghost, kind_gh])
    for part, pieces in enumerate((
        (red_r[0:3, :], kind_r[0:1], red_l[0:3, :], kind_l[0:1]),
        (red_r[3:6, :], kind_r[1:2], red_l[3:6, :], kind_l[1:2]),
        (ghost_r, kind_rg, ghost_l, kind_lg),
    )):
        rest = jnp.concatenate(list(pieces), axis=0)
        layers = []
        for _ in range(3):
            layer = rest.astype(BF16).astype(F32)
            layers.append(layer)
            rest = rest - layer
        col = jnp.transpose(jnp.concatenate(layers + [jnp.zeros((CH - 24, H), F32)], axis=0)).astype(BF16)
        spread = fast_dot(col, pick_v[...])
        for c in range(4):
            ggb[c, pl.ds(part * H, H), :] = spread[:, c * H : c * H + H]

    def ghost_rows(i, carry):
        rows = 32
        base = pl.multiple_of(i * rows, rows)
        dx, dy, dz = [ggb[c, pl.ds(base, rows), :] - ceng[c : c + 1, :] for c in range(3)]
        kind = ggb[3, pl.ds(base, rows), :]
        square = dx * dx + dy * dy + dz * dz + FLOOR
        rinv = lax.rsqrt(square)
        x = square * rinv * STEP
        rinvg_v[pl.ds(base, rows), :] = rinv
        c = cnt_gh[pl.ds(base, rows), :]
        sums = list(carry)
        for k in range(NB):
            off = x - CENTERS[k]
            a = c * jnp.exp2(-(off * off))
            zg_v[pl.ds(k * E + base, rows), :] = a * off
            s = a * kind
            sums[k] = sums[k] + folded(a)
            sums[NB + k] = sums[NB + k] + folded(s)
        return tuple(sums)

    sums = lax.fori_loop(0, 2 * G // 16, pair_rows(A), sums, unroll=UNROLL)
    gsums = tuple(jnp.zeros((8, H), F32) for _ in range(2 * NB))
    gsums = lax.fori_loop(0, E // 32, ghost_rows, gsums, unroll=UNROLL)

    stacked = jnp.concatenate(
        [jnp.concatenate(sums[0::2], axis=0), jnp.concatenate(sums[1::2], axis=0),
         jnp.concatenate(gsums, axis=0)], axis=1)
    u0 = left_dot(p0rt_cat[...], stacked)
    sig0 = 1.0 / (1.0 + jnp.exp(-u0))
    lt = left_dot(wmt_cat[...], h0_v[...] + u0 * sig0)

    message = None
    for k in range(0, NB, 2):
        parts = [split(lt * jnp.concatenate([w1bc[m]] * 3, axis=1)) for m in (k, k + 1)]
        hi, lo = [jnp.concatenate([part[j] for part in parts], axis=1) for j in range(2)]
        a_hi, a_lo = [
            jnp.concatenate([v[:, pl.ds(m * A, A)] for m in (k, k + 1)], axis=0) for v in (ah_v, al_v)]
        both = fast_dot(jnp.concatenate([hi, lo], axis=0), a_hi)
        term = both[:CH] + both[CH:] + fast_dot(hi, a_lo)
        message = term if message is None else message + term
    slope0[...] = jnp.transpose(sig0 * (1.0 + u0 * (1.0 - sig0)))
    lent = jnp.transpose(lt)
    l_hi, l_lo = split(lent)
    lcat = jnp.concatenate([l_hi, l_lo], axis=1)
    u1 = left_dot(wut_cat[...], message)
    sig1 = 1.0 / (1.0 + jnp.exp(-u1))
    wo2 = jnp.concatenate([wocol[...], wocol[...]], axis=1)
    gm1t = left_dot(wu_cat[...], wo2 * (sig1 * (1.0 + u1 * (1.0 - sig1))))
    gm1 = jnp.transpose(gm1t)
    for k in range(NB):
        hi, lo = split(gm1 * w1[k : k + 1, :])
        gs_v[pl.ds(k * A, A), pl.ds(0, CH)] = hi
        gs_v[pl.ds(k * A, A), pl.ds(CH, CH)] = lo
    both = fast_dot(ah_v[...], gs_v[...])
    both = both + fast_dot(al_v[...], gs_v[...])
    dl = both[:, :CH] + both[:, CH:]

    def radial_grad(ks, rows):
        for k in ks:
            w = w1bc[k]
            hi, lo = split(gm1t * jnp.concatenate([w, w], axis=1))
            first_row, last_row = rows
            da = fast_dot(lcat[first_row:last_row], jnp.concatenate([hi, hi], axis=0))
            da = da + fast_dot(l_hi[first_row:last_row], lo)
            at = pl.ds(first_row, last_row - first_row)
            term = da * z_v[pl.ds(k * E + first_row, last_row - first_row), :]
            q_v[at, :] = term if k == 0 else q_v[at, :] + term

    ghosts = (A, E)
    radial_grad((0, 1, 2), ghosts)
    gh1 = wide_dot(dl, wmt_w[...])
    radial_grad((3, 4, 5), ghosts)
    gh1 = jnp.concatenate([gh1[:A] + wo_v[...], gh1[A:]], axis=0)
    hi, lo = split(gh1 * slope0[...])
    p0c = p0_cat[...]
    db = fast_dot_nt(p0c, jnp.concatenate([hi, hi], axis=1)) + fast_dot_nt(p0c[:, :CH], lo)
    radial_grad((6, 7), ghosts)
    dbs[...] = jnp.concatenate([db[0:NB], db[0:NB] + db[NB : 2 * NB]], axis=0)

    factor = -2.0 / (0.2 * ROOT)

    def force_rows(start):
        rows = 16

        def step(i, carry):
            base = pl.multiple_of(start + i * rows, rows)
            at = pl.ds(base, rows)
            kind = gb[3, at, :] > 0.5
            new = list(carry)
            folds = [None] * 3
            for half in range(2):
                lanes = pl.ds(half * H, H)
                q = q_v[at, lanes]
                for k in range(NB):
                    coef = jnp.where(kind, dbs[NB + k : NB + k + 1, lanes], dbs[k : k + 1, lanes])
                    q = q + coef * z_v[pl.ds(k * E + base, rows), lanes]
                g = q * rinv_v[at, lanes] * factor
                for c in range(3):
                    f = g * (gb[c, at, :] - cen[c : c + 1, lanes])
                    folds[c] = f if half == 0 else folds[c] + f
                    new[2 * c + half] = new[2 * c + half] + folded(f)
            for c in range(3):
                fold_v[c, at, :] = folds[c]
            return tuple(new)

        return step

    def ghost_force(i, carry):
        rows = 32
        base = pl.multiple_of(i * rows, rows)
        kind = ggb[3, pl.ds(base, rows), :] > 0.5
        q = None
        for k in range(NB):
            coef = jnp.where(kind, dbs[NB + k : NB + k + 1, A:], dbs[k : k + 1, A:])
            term = coef * zg_v[pl.ds(k * E + base, rows), :]
            q = term if q is None else q + term
        g = q * rinvg_v[pl.ds(base, rows), :] * factor
        new = []
        for c in range(3):
            f = g * (ggb[c, pl.ds(base, rows), :] - ceng[c : c + 1, :])
            foldg_v[c, pl.ds(base, rows), :] = f
            new.append(carry[c] + folded(f))
        return tuple(new)

    def row_sums(start):
        return jnp.concatenate(
            [jnp.sum(jnp.transpose(fold_v[c, pl.ds(start, H), :]), axis=0, keepdims=True)
             for c in range(3)], axis=0)

    def ghost_sums(start):
        turned = [jnp.transpose(foldg_v[c, pl.ds(start, H), :]) for c in range(3)]
        return [
            jnp.concatenate([jnp.sum(t[G * part : G * part + G], axis=0, keepdims=True) for t in turned], axis=0)
            for part in range(2)
        ]

    gpulls = tuple(jnp.zeros((8, H), F32) for _ in range(3))
    gpulls = lax.fori_loop(0, E // 32, ghost_force, gpulls, unroll=UNROLL)
    r_end, l_end = ghost_sums(2 * H)
    tx_rr[...] = r_end
    tx_ll[...] = l_end
    r_low, l_low = ghost_sums(0)
    fifth = [
        side_copy(src, dst, s5.at[i], r5.at[i], side)
        for i, (src, dst, side) in enumerate((
            (tx_rr, rx_ll, right2), (tx_ll, rx_rr, left2), (tx_r, rx_l, right), (tx_l, rx_r, left)))
    ]
    for copy in fifth[:2]:
        copy.start()
    pulls = tuple(jnp.zeros((8, H), F32) for _ in range(6))
    pulls = lax.fori_loop(0, 2 * G // 16, force_rows(A), pulls, unroll=UNROLL)
    lent_pull = row_sums(A) - jnp.concatenate([jnp.sum(v, axis=0, keepdims=True) for v in gpulls], axis=0)
    r_high, l_high = ghost_sums(H)
    tx_r[...] = jnp.concatenate([r_low + jnp.where(low, lent_pull, 0.0), r_high], axis=0)
    tx_l[...] = jnp.concatenate([l_low, l_high + jnp.where(low, 0.0, lent_pull)], axis=0)
    for copy in fifth[2:]:
        copy.start()
    radial_grad(range(NB), (0, A))
    pulls = lax.fori_loop(0, A // 16, force_rows(0), pulls, unroll=UNROLL)
    centre = [jnp.sum(v, axis=0, keepdims=True) for v in pulls]
    lower = jnp.concatenate(centre[0::2], axis=0) - row_sums(0) - jnp.where(low, l_end, 0.0)
    upper = jnp.concatenate(centre[1::2], axis=0) - row_sums(H) - jnp.where(low, 0.0, r_end)
    for copy in fifth:
        copy.wait_recv()
    lower = lower - jnp.where(low, rx_ll[...], 0.0)
    upper = upper - jnp.where(low, 0.0, rx_rr[...])
    pull = jnp.concatenate([lower, upper], axis=0) - (rx_l[...] + rx_r[...])
    tx6[...] = pull
    last = {lag: bead_copy(tx6, rx6.at[lag], s6.at[lag], r6.at[lag], lag) for lag in lags}
    for lag in lags:
        last[lag].start()
    for copy in list(first.values()) + aux + second + fifth:
        copy.wait_send()
    ratio = beads / reduced
    totals = [ratio * table_value(-j, beads, reduced) * pull for j in range(own)]
    for lag in reversed(lags):
        last[lag].wait_recv()
        arrived = rx6[lag]
        for j in range(own):
            totals[j] = totals[j] + ratio * table_value(-own * lag - j, beads, reduced) * arrived
    for c in range(3):
        for half in range(2):
            row = 3 * half + c
            out_ref[c, :, half * H : half * H + H] = jnp.concatenate(
                [totals[j][row : row + 1] for j in range(own)], axis=0)
    for copy in last.values():
        copy.wait_send()


def solution(mesh):
    nb, ns = mesh.shape["bead"], mesh.shape["space"]

    def on_device(positions, species, neighbors, counts, send_rows, embed, w_radial, w_msg, w_upd, w_out):
        own = positions.shape[0]
        dma = pltpu.SemaphoreType.DMA

        def f32(*dims):
            return pltpu.VMEM(dims, F32)

        def i32(*dims):
            return pltpu.VMEM(dims, jnp.int32)

        def b16(*dims):
            return pltpu.VMEM(dims, BF16)

        scratch = [
            f32(3, own, A), i32(2, H), i32(K, A), i32(2, H), i32(1, H), f32(2, CH), f32(2, NB, CH),
            f32(2, CH, CH), f32(2, CH, CH), f32(1, CH),
            f32(nb, 6, H), f32(nb, 6, H),
            i32(2, H), i32(1, H), i32(2, H), i32(K, H), i32(2, H), i32(1, H), i32(2, H), i32(K, H),
            i32(2, H), i32(1, H), i32(2, H), i32(1, H),
            f32(6, H), f32(6, H), f32(6, H), f32(6, H), f32(6, H),
            i32(K, A), i32(K, H), f32(E, A), f32(E, H), f32(4, E, H), f32(4, E, H), f32(8, A), f32(8, H),
            f32(NB, CH, H), f32(CH, CH),
            b16(CH, 2 * CH), b16(2 * NB, 2 * CH), b16(CH, 2 * CH), b16(2 * CH, 2 * CH),
            b16(CH, 2 * CH), b16(CH, 2 * CH),
            f32(CH, E), f32(E, CH), b16(E, NB * A), b16(E, NB * A), f32(NB * E, A), f32(NB * E, H),
            f32(E, A), f32(E, H), b16(NB * A, 2 * CH), f32(E, A),
            b16(CH, 4 * H), f32(2 * NB, E), f32(3, E, H), f32(3, E, H),
            f32(6, H), f32(6, H), f32(3, H), f32(3, H), f32(6, H), f32(6, H), f32(3, H), f32(3, H),
            f32(6, H), f32(nb, 6, H),
            dma((10,)), dma((nb,)), dma((nb,)), dma((12,)), dma((12,)), dma((4,)), dma((4,)), dma((4,)), dma((4,)),
            dma((nb,)), dma((nb,)),
        ]
        forces = pl.pallas_call(
            functools.partial(kernel, nb, ns, own),
            out_shape=jax.ShapeDtypeStruct((3, own, A), F32),
            in_specs=[pl.BlockSpec(memory_space=pltpu.HBM)] * 10,
            out_specs=pl.BlockSpec(memory_space=pltpu.VMEM),
            scratch_shapes=scratch,
            compiler_params=pltpu.CompilerParams(
                collective_id=0, has_side_effects=True, vmem_limit_bytes=40 * 1024 * 1024),
        )(
            *[pltpu.with_memory_space_constraint(v, pltpu.HBM) for v in (positions.transpose(1, 0, 2), species.reshape(2, H), neighbors, counts.reshape(2, H),
            send_rows.reshape(1, H), embed, w_radial, w_msg, w_upd, w_out.reshape(1, CH))],
        )
        return forces.transpose(1, 0, 2)

    return jax.shard_map(
        on_device,
        mesh=mesh,
        in_specs=(
            P("bead", None, "space"), P("space"), P(None, "space"), P("space"), P("space"),
            P(), P(), P(), P(), P(),
        ),
        out_specs=P("bead", None, "space"),
        check_vma=False,
    )
```

```python
import functools
import math

import jax
import jax.numpy as jnp
from jax import lax
from jax.experimental import pallas as pl
from jax.experimental.pallas import tpu as pltpu
from jax.sharding import PartitionSpec as P

MESH = pl.DeviceIdType.MESH
HI = lax.Precision.HIGHEST
F32 = jnp.float32
BF16 = jnp.bfloat16

NB = 8
CH = 128
A = 256
G = 64
E = A + 2 * G
K = 32
H = 128
ROOT = math.sqrt(math.log2(math.e))
STEP = ROOT / 0.2
CENTERS = tuple(STEP * 1.5 * b / (NB - 1) for b in range(NB))
FLOOR = 0.01
UNROLL = 4


def by_distance(nb):
    def far(lag):
        dz, dx = lag % 4, lag // 4
        return -(2 * min(dz, 4 - dz) + min(dx, 4 - dx))

    return sorted(range(1, nb), key=far)


def table_value(lag, beads, reduced):
    t = lag / beads
    total = 1.0 + math.cos(math.pi * reduced * t)
    for m in range(1, reduced // 2):
        total += 2.0 * math.cos(2.0 * math.pi * m * t)
    return total / beads


def split(v):
    hi = v.astype(BF16)
    lo = (v - hi.astype(F32)).astype(BF16)
    return hi, lo


def exact_dot(a, b):
    return jnp.dot(a, b, precision=HI, preferred_element_type=F32)


def fast_dot(a, b):
    return jnp.dot(a, b, preferred_element_type=F32)


def wide(w):
    hi, lo = split(w)
    row = jnp.concatenate([hi, lo], axis=1)
    return jnp.concatenate([row, row], axis=0)


def wide_dot(a, w):
    hi, lo = split(a)
    both = fast_dot(jnp.concatenate([hi, lo], axis=1), w)
    return both[:, :CH] + both[:, CH:]


def beside(w):
    hi, lo = split(w)
    return jnp.concatenate([hi, lo], axis=1)


def left_dot(w, a):
    hi, lo = split(a)
    return fast_dot(w, jnp.concatenate([hi, hi], axis=0)) + fast_dot(w[:, :CH], lo)


def fast_dot_nt(a, b):
    return lax.dot_general(a, b, (((1,), (1,)), ((), ())), preferred_element_type=F32)


def kernel(
    nb, ns, own,
    pos_h, spc_h, nbr_h, cnt_h, snd_h, emb_h, wr_h, wm_h, wu_h, wo_h,
    out_ref,
    pos_v, spc_v, nbr_v, cnt_v, snd_v, emb_v, wr_v, wm_v, wu_v, wo_v,
    tx1, rx1,
    spc_r, snd_r, cnt_r, nbr_r, spc_l, snd_l, cnt_l, nbr_l, spc_rr, snd_rr, spc_ll, snd_ll,
    red_v, red_r, red_l, red_rr, red_ll,
    idx_v, idx_g, cnt_mat, cnt_gh, gb, ggb, cen, ceng, w1bc, wocol,
    p0rt_cat, p0_cat, wmt_cat, wmt_w, wu_cat, wut_cat,
    h0_v, slope0, ah_v, al_v, z_v, zg_v, rinv_v, rinvg_v, gs_v, q_v,
    pick_v, dbs, fold_v, foldg_v, tx_r, tx_l, tx_rr, tx_ll, rx_r, rx_l, rx_rr, rx_ll, tx6, rx6,
    load_sem, s1, r1, sa, ra, s2, r2, s5, r5, s6, r6,
):
    beads, reduced = nb * own, nb
    scale = K ** -0.5
    b = lax.axis_index("bead")
    d = lax.axis_index("space")
    left = lax.rem(d + (ns - 1), ns)
    right = lax.rem(d + 1, ns)
    left2 = lax.rem(d + (ns - 2), ns)
    right2 = lax.rem(d + 2, ns)
    peers = [lax.rem(b + lag, nb) for lag in range(nb)]
    lags = by_distance(nb)

    def bead_copy(src, dst, ss, rs, lag):
        return pltpu.make_async_remote_copy(
            src_ref=src, dst_ref=dst, send_sem=ss, recv_sem=rs,
            device_id=peers[lag] * ns + d, device_id_type=pl.DeviceIdType.LOGICAL)

    def side_copy(src, dst, ss, rs, side):
        return pltpu.make_async_remote_copy(
            src_ref=src, dst_ref=dst, send_sem=ss, recv_sem=rs,
            device_id=b * ns + side, device_id_type=pl.DeviceIdType.LOGICAL)

    barrier = pltpu.get_barrier_semaphore()
    for lag in lags:
        pl.semaphore_signal(barrier, inc=1, device_id=peers[lag] * ns + d, device_id_type=pl.DeviceIdType.LOGICAL)
    for side in (left, right, left2, right2):
        pl.semaphore_signal(barrier, inc=1, device_id=b * ns + side, device_id_type=pl.DeviceIdType.LOGICAL)

    loads = []
    for i, (src, dst) in enumerate((
        (pos_h, pos_v), (spc_h, spc_v), (snd_h, snd_v), (nbr_h, nbr_v), (cnt_h, cnt_v),
        (emb_h, emb_v), (wr_h, wr_v), (wm_h, wm_v), (wu_h, wu_v), (wo_h, wo_v),
    )):
        copy = pltpu.make_async_copy(src, dst, load_sem.at[i])
        copy.start()
        loads.append(copy)

    loads[0].wait()
    packed = []
    for j in range(own):
        packed.append(jnp.concatenate(
            [pos_v[c, j : j + 1, half * H : half * H + H] for half in range(2) for c in range(3)], axis=0))
    for lag in range(nb):
        total = None
        for j in range(own):
            term = table_value(own * lag - j, beads, reduced) * packed[j]
            total = term if total is None else total + term
        tx1[lag] = total
    for copy in loads[1:5]:
        copy.wait()
    pl.semaphore_wait(barrier, nb + 3)

    first = {lag: bead_copy(tx1.at[lag], rx1.at[lag], s1.at[lag], r1.at[lag], lag) for lag in lags}
    for lag in lags:
        first[lag].start()
    near = pl.ds(0, H)
    far = pl.ds(H, H)
    aux = [
        side_copy(src, dst, sa.at[i], ra.at[i], side)
        for i, (src, dst, side) in enumerate((
            (nbr_v.at[:, near], nbr_r, left), (nbr_v.at[:, far], nbr_l, right),
            (cnt_v, cnt_r, left), (cnt_v, cnt_l, right),
            (spc_v, spc_r, left), (spc_v, spc_l, right), (spc_v, spc_rr, left2), (spc_v, spc_ll, right2),
            (snd_v, snd_r, left), (snd_v, snd_l, right), (snd_v, snd_rr, left2), (snd_v, snd_ll, right2),
        ))
    ]
    for copy in aux:
        copy.start()

    def rows_named(n, count):
        n = jnp.where(n >= A + G, n - G, jnp.where(n >= A, n + G, n))
        slot = lax.broadcasted_iota(jnp.int32, n.shape, 0)
        return jnp.where(slot < count, n, -1)

    def count_rows(idx, mat, width, rows):
        def step(i, carry):
            base = pl.multiple_of(i * rows, rows)
            row = lax.broadcasted_iota(jnp.int32, (rows, width), 0) + base
            acc = jnp.zeros((rows, width), F32)
            for k in range(K):
                acc = acc + jnp.where(idx[k : k + 1, :] == row, 1.0, 0.0)
            mat[pl.ds(base, rows), :] = acc
            return carry

        lax.fori_loop(0, E // rows, step, 0)

    idx_v[...] = rows_named(nbr_v[...], jnp.concatenate([cnt_v[0:1, :], cnt_v[1:2, :]], axis=1))
    count_rows(idx_v, cnt_mat, A, 32)

    for copy in loads[5:]:
        copy.wait()
    zeros6 = jnp.zeros((6, CH), F32)
    emb8 = jnp.concatenate([emb_v[...], zeros6], axis=0)
    table = exact_dot(emb8, wm_v[0])
    w0 = wr_v[0] * scale
    rows0 = jnp.concatenate([w0 * table[0:1], w0 * (table[1:2] - table[0:1])], axis=0)
    p0 = exact_dot(rows0, wu_v[0])
    p0_hi, p0_lo = split(p0)
    p0_cat[...] = jnp.concatenate([p0_hi, p0_lo], axis=1)
    p0rt_cat[...] = beside(jnp.transpose(jnp.concatenate(
        [jnp.broadcast_to(p0[j : j + 1, :], (8, CH)) for j in range(2 * NB)], axis=0)))
    w1 = wr_v[1] * scale
    w1t = jnp.transpose(jnp.concatenate([w1, jnp.zeros((CH - NB, CH), F32)], axis=0))
    for k in range(NB):
        w1bc[k] = jnp.broadcast_to(w1t[:, k : k + 1], (CH, H))
    wm_turned = jnp.transpose(wm_v[1])
    wmt_cat[...] = beside(wm_turned)
    wmt_w[...] = wide(wm_turned)
    wu_cat[...] = beside(wu_v[1])
    wut_cat[...] = beside(jnp.transpose(wu_v[1]))
    wocol[...] = jnp.transpose(jnp.broadcast_to(wo_v[...], (CH, CH)))

    lane = lax.broadcasted_iota(jnp.int32, (1, H), 1)
    low = lane < G

    row = lax.broadcasted_iota(jnp.int32, (CH, 4 * H), 0)
    spot = lax.broadcasted_iota(jnp.int32, (CH, 4 * H), 1)
    value = spot // H + jnp.where(spot % H < G, 0, 4)
    pick_v[...] = jnp.where((row < 24) & (row % 8 == value), 1.0, 0.0).astype(BF16)

    red = tx1[0]
    for lag in lags:
        first[lag].wait_recv()
        red = red + rx1[lag]
    red_v[...] = red
    second = [
        side_copy(red_v, dst, s2.at[i], r2.at[i], side)
        for i, (dst, side) in enumerate(((red_rr, left2), (red_ll, right2), (red_r, left), (red_l, right)))
    ]
    for copy in second:
        copy.start()

    for copy in aux:
        copy.wait_recv()
    idx_g[...] = rows_named(
        jnp.where(low, nbr_r[...], nbr_l[...]), jnp.where(low, cnt_r[0:1, :], cnt_l[1:2, :]))
    count_rows(idx_g, cnt_gh, H, 64)
    natural = lax.broadcasted_iota(jnp.int32, (H, H), 0)

    def reorder(from_right, from_left, rows):
        order = jnp.where(low, from_right, from_left - (A - H))
        return fast_dot(jnp.where(natural == order, 1.0, 0.0).astype(BF16), rows)

    cnt_mat[pl.ds(A, 2 * G), :] = reorder(snd_r[...], snd_l[...], cnt_mat[pl.ds(A, 2 * G), :].astype(BF16))
    rows_gh = cnt_gh[pl.ds(A, 2 * G), :].astype(BF16)
    cnt_gh[pl.ds(A, 2 * G), :] = jnp.where(
        low, reorder(snd_rr[...], snd_v[...], rows_gh), reorder(snd_v[...], snd_ll[...], rows_gh))
    kind_own = spc_v[...].astype(F32)
    kind_r, kind_l = spc_r[...].astype(F32), spc_l[...].astype(F32)
    kind_gh = jnp.where(low, kind_r[0:1], kind_l[1:2])
    kind_rg = jnp.where(low, spc_rr[0:1, :].astype(F32), kind_own[1:2])
    kind_lg = jnp.where(low, kind_own[0:1], spc_ll[1:2, :].astype(F32))
    zrest = jnp.zeros((CH - 4, H), F32)
    kinds = [jnp.transpose(jnp.broadcast_to(emb_v[t : t + 1, :], (H, CH))) for t in range(2)]
    for part, kind in enumerate((kind_own[0:1], kind_own[1:2], kind_gh)):
        h0_v[:, pl.ds(part * H, H)] = jnp.where(kind > 0.5, kinds[1], kinds[0])
    cen[...] = jnp.concatenate(
        [jnp.concatenate([red[0:3], red[3:6]], axis=1), jnp.zeros((5, A), F32)], axis=0)

    def spread_rows(part, pieces):
        col = jnp.transpose(jnp.concatenate(pieces + [zrest], axis=0))
        for c in range(4):
            gb[c, pl.ds(part * H, H), :] = jnp.broadcast_to(col[:, c : c + 1], (H, H))

    for half in range(2):
        spread_rows(half, [red[3 * half : 3 * half + 3], kind_own[half : half + 1]])

    def folded(v):
        total = v[0:8]
        for r in range(8, v.shape[0], 8):
            total = total + v[r : r + 8]
        return total

    def pair_rows(start):
        rows = 16

        def step(i, carry):
            base = pl.multiple_of(start + i * rows, rows)
            at = pl.ds(base, rows)
            gx, gy, gz, kind = [gb[c, at, :] for c in range(4)]
            sums = list(carry)
            for half in range(2):
                lanes = pl.ds(half * H, H)
                dx, dy, dz = gx - cen[0:1, lanes], gy - cen[1:2, lanes], gz - cen[2:3, lanes]
                square = dx * dx + dy * dy + dz * dz + FLOOR
                rinv = lax.rsqrt(square)
                x = square * rinv * STEP
                rinv_v[at, lanes] = rinv
                c = cnt_mat[at, lanes]
                for k in range(NB):
                    off = x - CENTERS[k]
                    a = c * jnp.exp2(-(off * off))
                    hi, lo = split(a)
                    spot = pl.ds(k * A + half * H, H)
                    ah_v[at, spot] = hi
                    al_v[at, spot] = lo
                    z_v[pl.ds(k * E + base, rows), lanes] = a * off
                    sums[2 * k + half] = sums[2 * k + half] + folded(a)
                    j = 2 * NB + 2 * k + half
                    sums[j] = sums[j] + folded(a * kind)
            return tuple(sums)

        return step

    sums = tuple(jnp.zeros((8, H), F32) for _ in range(4 * NB))
    sums = lax.fori_loop(0, A // 16, pair_rows(0), sums, unroll=UNROLL)
    for copy in second:
        copy.wait_recv()

    def shifted(at_left, at_right, values):
        shift = jnp.where(low, jnp.where(at_right, float(ns), 0.0), jnp.where(at_left, -float(ns), 0.0))
        first_row = lax.broadcasted_iota(jnp.int32, (3, H), 0) == 0
        return values + jnp.where(first_row, shift, 0.0)

    borrowed = jnp.where(low, red_r[0:3, :], red_l[3:6, :])
    ceng[...] = jnp.concatenate([borrowed, jnp.zeros((5, H), F32)], axis=0)
    ghost = shifted(d == 0, d == ns - 1, borrowed)
    ghost_r = shifted(right == 0, right == ns - 1, jnp.where(low, red_rr[0:3, :], red[3:6]))
    ghost_l = shifted(left == 0, left == ns - 1, jnp.where(low, red[0:3], red_ll[3:6, :]))
    spread_rows(2, [ghost, kind_gh])
    for part, pieces in enumerate((
        (red_r[0:3, :], kind_r[0:1], red_l[0:3, :], kind_l[0:1]),
        (red_r[3:6, :], kind_r[1:2], red_l[3:6, :], kind_l[1:2]),
        (ghost_r, kind_rg, ghost_l, kind_lg),
    )):
        rest = jnp.concatenate(list(pieces), axis=0)
        layers = []
        for _ in range(3):
            layer = rest.astype(BF16).astype(F32)
            layers.append(layer)
            rest = rest - layer
        col = jnp.transpose(jnp.concatenate(layers + [jnp.zeros((CH - 24, H), F32)], axis=0)).astype(BF16)
        spread = fast_dot(col, pick_v[...])
        for c in range(4):
            ggb[c, pl.ds(part * H, H), :] = spread[:, c * H : c * H + H]

    def ghost_rows(i, carry):
        rows = 32
        base = pl.multiple_of(i * rows, rows)
        dx, dy, dz = [ggb[c, pl.ds(base, rows), :] - ceng[c : c + 1, :] for c in range(3)]
        kind = ggb[3, pl.ds(base, rows), :]
        square = dx * dx + dy * dy + dz * dz + FLOOR
        rinv = lax.rsqrt(square)
        x = square * rinv * STEP
        rinvg_v[pl.ds(base, rows), :] = rinv
        c = cnt_gh[pl.ds(base, rows), :]
        sums = list(carry)
        for k in range(NB):
            off = x - CENTERS[k]
            a = c * jnp.exp2(-(off * off))
            zg_v[pl.ds(k * E + base, rows), :] = a * off
            s = a * kind
            sums[k] = sums[k] + folded(a)
            sums[NB + k] = sums[NB + k] + folded(s)
        return tuple(sums)

    sums = lax.fori_loop(0, 2 * G // 16, pair_rows(A), sums, unroll=UNROLL)
    gsums = tuple(jnp.zeros((8, H), F32) for _ in range(2 * NB))
    gsums = lax.fori_loop(0, E // 32, ghost_rows, gsums, unroll=UNROLL)

    stacked = jnp.concatenate(
        [jnp.concatenate(sums[0::2], axis=0), jnp.concatenate(sums[1::2], axis=0),
         jnp.concatenate(gsums, axis=0)], axis=1)
    u0 = left_dot(p0rt_cat[...], stacked)
    sig0 = 1.0 / (1.0 + jnp.exp(-u0))
    lt = left_dot(wmt_cat[...], h0_v[...] + u0 * sig0)

    message = None
    for k in range(0, NB, 2):
        parts = [split(lt * jnp.concatenate([w1bc[m]] * 3, axis=1)) for m in (k, k + 1)]
        hi, lo = [jnp.concatenate([part[j] for part in parts], axis=1) for j in range(2)]
        a_hi, a_lo = [
            jnp.concatenate([v[:, pl.ds(m * A, A)] for m in (k, k + 1)], axis=0) for v in (ah_v, al_v)]
        both = fast_dot(jnp.concatenate([hi, lo], axis=0), a_hi)
        term = both[:CH] + both[CH:] + fast_dot(hi, a_lo)
        message = term if message is None else message + term
    slope0[...] = jnp.transpose(sig0 * (1.0 + u0 * (1.0 - sig0)))
    lent = jnp.transpose(lt)
    l_hi, l_lo = split(lent)
    lcat = jnp.concatenate([l_hi, l_lo], axis=1)
    u1 = left_dot(wut_cat[...], message)
    sig1 = 1.0 / (1.0 + jnp.exp(-u1))
    wo2 = jnp.concatenate([wocol[...], wocol[...]], axis=1)
    gm1t = left_dot(wu_cat[...], wo2 * (sig1 * (1.0 + u1 * (1.0 - sig1))))
    gm1 = jnp.transpose(gm1t)
    for k in range(NB):
        hi, lo = split(gm1 * w1[k : k + 1, :])
        gs_v[pl.ds(k * A, A), pl.ds(0, CH)] = hi
        gs_v[pl.ds(k * A, A), pl.ds(CH, CH)] = lo
    both = fast_dot(ah_v[...], gs_v[...])
    both = both + fast_dot(al_v[...], gs_v[...])
    dl = both[:, :CH] + both[:, CH:]

    def radial_grad(ks, rows):
        for k in ks:
            w = w1bc[k]
            hi, lo = split(gm1t * jnp.concatenate([w, w], axis=1))
            first_row, last_row = rows
            da = fast_dot(lcat[first_row:last_row], jnp.concatenate([hi, hi], axis=0))
            da = da + fast_dot(l_hi[first_row:last_row], lo)
            at = pl.ds(first_row, last_row - first_row)
            term = da * z_v[pl.ds(k * E + first_row, last_row - first_row), :]
            q_v[at, :] = term if k == 0 else q_v[at, :] + term

    ghosts = (A, E)
    radial_grad((0, 1, 2), ghosts)
    gh1 = wide_dot(dl, wmt_w[...])
    radial_grad((3, 4, 5), ghosts)
    gh1 = jnp.concatenate([gh1[:A] + wo_v[...], gh1[A:]], axis=0)
    hi, lo = split(gh1 * slope0[...])
    p0c = p0_cat[...]
    db = fast_dot_nt(p0c, jnp.concatenate([hi, hi], axis=1)) + fast_dot_nt(p0c[:, :CH], lo)
    radial_grad((6, 7), ghosts)
    dbs[...] = jnp.concatenate([db[0:NB], db[0:NB] + db[NB : 2 * NB]], axis=0)

    factor = -2.0 / (0.2 * ROOT)

    def force_rows(start):
        rows = 16

        def step(i, carry):
            base = pl.multiple_of(start + i * rows, rows)
            at = pl.ds(base, rows)
            kind = gb[3, at, :] > 0.5
            new = list(carry)
            folds = [None] * 3
            for half in range(2):
                lanes = pl.ds(half * H, H)
                q = q_v[at, lanes]
                for k in range(NB):
                    coef = jnp.where(kind, dbs[NB + k : NB + k + 1, lanes], dbs[k : k + 1, lanes])
                    q = q + coef * z_v[pl.ds(k * E + base, rows), lanes]
                g = q * rinv_v[at, lanes] * factor
                for c in range(3):
                    f = g * (gb[c, at, :] - cen[c : c + 1, lanes])
                    folds[c] = f if half == 0 else folds[c] + f
                    new[2 * c + half] = new[2 * c + half] + folded(f)
            for c in range(3):
                fold_v[c, at, :] = folds[c]
            return tuple(new)

        return step

    def ghost_force(i, carry):
        rows = 32
        base = pl.multiple_of(i * rows, rows)
        kind = ggb[3, pl.ds(base, rows), :] > 0.5
        q = None
        for k in range(NB):
            coef = jnp.where(kind, dbs[NB + k : NB + k + 1, A:], dbs[k : k + 1, A:])
            term = coef * zg_v[pl.ds(k * E + base, rows), :]
            q = term if q is None else q + term
        g = q * rinvg_v[pl.ds(base, rows), :] * factor
        new = []
        for c in range(3):
            f = g * (ggb[c, pl.ds(base, rows), :] - ceng[c : c + 1, :])
            foldg_v[c, pl.ds(base, rows), :] = f
            new.append(carry[c] + folded(f))
        return tuple(new)

    def row_sums(start):
        return jnp.concatenate(
            [jnp.sum(jnp.transpose(fold_v[c, pl.ds(start, H), :]), axis=0, keepdims=True)
             for c in range(3)], axis=0)

    def ghost_sums(start):
        turned = [jnp.transpose(foldg_v[c, pl.ds(start, H), :]) for c in range(3)]
        return [
            jnp.concatenate([jnp.sum(t[G * part : G * part + G], axis=0, keepdims=True) for t in turned], axis=0)
            for part in range(2)
        ]

    gpulls = tuple(jnp.zeros((8, H), F32) for _ in range(3))
    gpulls = lax.fori_loop(0, E // 32, ghost_force, gpulls, unroll=UNROLL)
    r_end, l_end = ghost_sums(2 * H)
    tx_rr[...] = r_end
    tx_ll[...] = l_end
    r_low, l_low = ghost_sums(0)
    fifth = [
        side_copy(src, dst, s5.at[i], r5.at[i], side)
        for i, (src, dst, side) in enumerate((
            (tx_rr, rx_ll, right2), (tx_ll, rx_rr, left2), (tx_r, rx_l, right), (tx_l, rx_r, left)))
    ]
    for copy in fifth[:2]:
        copy.start()
    pulls = tuple(jnp.zeros((8, H), F32) for _ in range(6))
    pulls = lax.fori_loop(0, 2 * G // 16, force_rows(A), pulls, unroll=UNROLL)
    lent_pull = row_sums(A) - jnp.concatenate([jnp.sum(v, axis=0, keepdims=True) for v in gpulls], axis=0)
    r_high, l_high = ghost_sums(H)
    tx_r[...] = jnp.concatenate([r_low + jnp.where(low, lent_pull, 0.0), r_high], axis=0)
    tx_l[...] = jnp.concatenate([l_low, l_high + jnp.where(low, 0.0, lent_pull)], axis=0)
    for copy in fifth[2:]:
        copy.start()
    radial_grad(range(NB), (0, A))
    pulls = lax.fori_loop(0, A // 16, force_rows(0), pulls, unroll=UNROLL)
    centre = [jnp.sum(v, axis=0, keepdims=True) for v in pulls]
    lower = jnp.concatenate(centre[0::2], axis=0) - row_sums(0) - jnp.where(low, l_end, 0.0)
    upper = jnp.concatenate(centre[1::2], axis=0) - row_sums(H) - jnp.where(low, 0.0, r_end)
    for copy in fifth:
        copy.wait_recv()
    lower = lower - jnp.where(low, rx_ll[...], 0.0)
    upper = upper - jnp.where(low, 0.0, rx_rr[...])
    pull = jnp.concatenate([lower, upper], axis=0) - (rx_l[...] + rx_r[...])
    tx6[...] = pull
    last = {lag: bead_copy(tx6, rx6.at[lag], s6.at[lag], r6.at[lag], lag) for lag in lags}
    for lag in lags:
        last[lag].start()
    for copy in list(first.values()) + aux + second + fifth:
        copy.wait_send()
    ratio = beads / reduced
    totals = [ratio * table_value(-j, beads, reduced) * pull for j in range(own)]
    for lag in reversed(lags):
        last[lag].wait_recv()
        arrived = rx6[lag]
        for j in range(own):
            totals[j] = totals[j] + ratio * table_value(-own * lag - j, beads, reduced) * arrived
    for c in range(3):
        for half in range(2):
            row = 3 * half + c
            out_ref[c, :, half * H : half * H + H] = jnp.concatenate(
                [totals[j][row : row + 1] for j in range(own)], axis=0)
    for copy in last.values():
        copy.wait_send()


def solution(mesh):
    nb, ns = mesh.shape["bead"], mesh.shape["space"]

    def on_device(positions, species, neighbors, counts, send_rows, embed, w_radial, w_msg, w_upd, w_out):
        own = positions.shape[0]
        dma = pltpu.SemaphoreType.DMA

        def f32(*dims):
            return pltpu.VMEM(dims, F32)

        def i32(*dims):
            return pltpu.VMEM(dims, jnp.int32)

        def b16(*dims):
            return pltpu.VMEM(dims, BF16)

        scratch = [
            f32(3, own, A), i32(2, H), i32(K, A), i32(2, H), i32(1, H), f32(2, CH), f32(2, NB, CH),
            f32(2, CH, CH), f32(2, CH, CH), f32(1, CH),
            f32(nb, 6, H), f32(nb, 6, H),
            i32(2, H), i32(1, H), i32(2, H), i32(K, H), i32(2, H), i32(1, H), i32(2, H), i32(K, H),
            i32(2, H), i32(1, H), i32(2, H), i32(1, H),
            f32(6, H), f32(6, H), f32(6, H), f32(6, H), f32(6, H),
            i32(K, A), i32(K, H), f32(E, A), f32(E, H), f32(4, E, H), f32(4, E, H), f32(8, A), f32(8, H),
            f32(NB, CH, H), f32(CH, CH),
            b16(CH, 2 * CH), b16(2 * NB, 2 * CH), b16(CH, 2 * CH), b16(2 * CH, 2 * CH),
            b16(CH, 2 * CH), b16(CH, 2 * CH),
            f32(CH, E), f32(E, CH), b16(E, NB * A), b16(E, NB * A), f32(NB * E, A), f32(NB * E, H),
            f32(E, A), f32(E, H), b16(NB * A, 2 * CH), f32(E, A),
            b16(CH, 4 * H), f32(2 * NB, E), f32(3, E, H), f32(3, E, H),
            f32(6, H), f32(6, H), f32(3, H), f32(3, H), f32(6, H), f32(6, H), f32(3, H), f32(3, H),
            f32(6, H), f32(nb, 6, H),
            dma((10,)), dma((nb,)), dma((nb,)), dma((12,)), dma((12,)), dma((4,)), dma((4,)), dma((4,)), dma((4,)),
            dma((nb,)), dma((nb,)),
        ]
        forces = pl.pallas_call(
            functools.partial(kernel, nb, ns, own),
            out_shape=jax.ShapeDtypeStruct((3, own, A), F32),
            in_specs=[pl.BlockSpec(memory_space=pltpu.HBM)] * 10,
            out_specs=pl.BlockSpec(memory_space=pltpu.VMEM),
            scratch_shapes=scratch,
            compiler_params=pltpu.CompilerParams(
                collective_id=0, has_side_effects=True, vmem_limit_bytes=40 * 1024 * 1024),
        )(
            *[pltpu.with_memory_space_constraint(v, pltpu.HBM) for v in (positions.transpose(1, 0, 2), species.reshape(2, H), neighbors, counts.reshape(2, H),
            send_rows.reshape(1, H), embed, w_radial, w_msg, w_upd, w_out.reshape(1, CH))],
        )
        return forces.transpose(1, 0, 2)

    return jax.shard_map(
        on_device,
        mesh=mesh,
        in_specs=(
            P("bead", None, "space"), P("space"), P(None, "space"), P("space"), P("space"),
            P(), P(), P(), P(), P(),
        ),
        out_specs=P("bead", None, "space"),
        check_vma=False,
    )
```
